32 devices in a mesh: dp: 4 (over y, core), seq: 8 (over z, x).
Axes of the slice: x: 2, y: 2, z: 4, core: 2. Of those that a mesh axis runs over, the one named last changes fastest.
Arguments:
- head_inputs: bfloat16 [4, 3072, 1024], P('dp', 'seq'), may hold values from -6 to 6
- gate_inputs: bfloat16 [4, 3072, 1024], P('dp', 'seq'), may hold values from -6 to 6
- state_proj: bfloat16 [4, 3072, 256], P('dp', 'seq'), may hold values from -2 to 2
- time_steps: float32 [4, 3072, 16], P('dp', 'seq'), may hold values from -4.7 to 4.7
- token_ids: int32 [4, 3072], P('dp', 'seq'), may hold values from 0 to 50279, as said below
- token_counts: int32 [4], replicated, may hold values from 1536 to 3072
- teacher_out: bfloat16 [4, 3072, 1024], P('dp', 'seq'), may hold values from -6 to 6
- out_weight: float32 [1024, 1024], P(('dp', 'seq')), may hold values from -0.1875 to 0.1875
- decay_log: float32 [16], replicated, may hold values from -6.5 to 1
- step_bias: float32 [16], replicated, may hold values from -5 to -3
- skip_gain: float32 [16], replicated, may hold values from 0.5 to 1.5
- norm_gain: float32 [1024], replicated, may hold values from 0.5 to 1.5
Outputs:
- losses: float32 [2], replicated
- new_weight: float32 [1024, 1024], P(('dp', 'seq'))
- new_decay: float32 [16], replicated
- new_bias: float32 [16], replicated
- new_skip: float32 [16], replicated
- new_gain: float32 [1024], replicated
The draws below stay inside these ranges and needn't reach their ends.
Inputs may be any that keep to these rules, and one draw needn't show every extreme that they name: `token_ids`: in each sequence exactly one position, never the first, holds id 0.
All inputs are finite; a program needn't handle non-finite values.
Results may differ from the reference program's by a relative error of at most 0.0003.
Values may be sent and summed in bfloat16 or wider, within the bound.
A program may use at most 192 MiB of HBM per device.

```python
import jax
import jax.numpy as jnp
from jax import lax

D = 1024
N = 128
VOCAB = 50280
H = 16
STEPS = 2
TOK_DEV = 384
SEQS = 4
LENGTH = 3072
DI = 1024
N_SEQ = 8


def draw_time_steps(key, part):
    noise_key, shift_key = jax.random.split(key)
    blocks = LENGTH // TOK_DEV
    offset = jax.random.uniform(shift_key, (SEQS, blocks, 1, H), jnp.float32, -0.7, 0.7)
    jitter = jnp.clip(jax.random.normal(noise_key, (SEQS, blocks, TOK_DEV, H), jnp.float32), -4.0, 4.0)
    return (jitter + offset).reshape(SEQS, LENGTH, H)


def draw_decay_log(key, part):
    pick_key, strong_key, weak_key = jax.random.split(key, 3)
    strong = jax.random.randint(pick_key, (H,), 0, 2) > 0
    slow_rate = jax.random.uniform(strong_key, (H,), jnp.float32, -6.5, -5.5)
    quick_rate = jax.random.uniform(weak_key, (H,), jnp.float32, 0.0, 1.0)
    return jnp.where(strong, slow_rate, quick_rate)


def draw_token_ids(key, part):
    token_key, reset_key = jax.random.split(key)
    token_draw = jax.random.randint(token_key, (SEQS, LENGTH), 1, VOCAB)
    reset_at = jax.random.randint(reset_key, (SEQS, 1), 1, LENGTH)
    return jnp.where(jnp.arange(LENGTH)[None, :] == reset_at, 0, token_draw).astype(jnp.int32)


def plant(drawn, stream_key, low, largest):
    place = [jax.random.randint(jax.random.fold_in(stream_key, axis), (), 0, length) for axis, length in enumerate(drawn.shape)]
    main_axis = drawn.shape.index(max(drawn.shape))
    beside = place[:main_axis] + [(place[main_axis] + 1) % drawn.shape[main_axis]] + place[main_axis + 1:]
    return drawn.at[tuple(place)].set(low).at[tuple(beside)].set(largest)


def spiked(result, own_key, source, target, parts, factor):
    owner, partner = [(jnp.arange(result.shape[axis_at]) // (result.shape[axis_at] // parts)).reshape([-1 if axis == axis_at else 1 for axis in range(result.ndim)]) for axis_at in (source, target)]
    chosen = jax.random.permutation(own_key, parts)[partner]
    strong = (owner == chosen) | (owner == (partner + parts // 2) % parts)
    return jnp.where(strong, factor * result, result)


def steps_of(own_key, dims, cuts, least, high):
    factor_of, own = 1.0, jax.random.fold_in(own_key, 6)
    for axis_at, blocks in cuts:
        steps = jnp.exp(jax.random.uniform(jax.random.fold_in(own, axis_at), (blocks,), jnp.float32, least / len(cuts), high / len(cuts)))
        factor_of = factor_of * jnp.repeat(steps, dims[axis_at] // blocks).reshape([-1 if axis == axis_at else 1 for axis in range(len(dims))])
    return factor_of


def scatter_about(stream_key, shape, scale, reach, cuts=(), kind=jnp.bfloat16):
    result = jax.random.normal(stream_key, shape, jnp.float32) * scale
    if len(cuts) > 0:
        result = steps_of(stream_key, shape, cuts, -0.22, 0.18) * result
    return jnp.clip(result, min=-reach, max=reach).astype(kind)


def gaussian_with(key, dims, scale, bound, cuts, heavy, dtype=jnp.bfloat16):
    entries = scale * jax.random.normal(key, dims, jnp.float32)
    if cuts:
        entries = entries * steps_of(key, dims, cuts, -0.22, 0.18)
    return jnp.clip(spiked(entries, jax.random.fold_in(key, 3), *heavy), -bound, bound).astype(dtype)


def setup_inputs(seed: int = 0) -> dict:
    arg_keys = jax.random.split(jax.random.key(seed), 13)
    return {
        "head_inputs": scatter_about(arg_keys[0], (SEQS, LENGTH, DI), 1.0, 6.0, ((0, 4), (1, 8))),
        "gate_inputs": gaussian_with(arg_keys[1], (SEQS, LENGTH, DI), 1.0, 6.0, ((0, 4), (1, 8)), (1, 2, 8, 2.0)),
        "state_proj": scatter_about(arg_keys[2], (SEQS, LENGTH, 2 * N), 0.3, 2.0, ((0, 4), (1, 8))),
        "time_steps": draw_time_steps(jax.random.fold_in(arg_keys[12], 71), 0),
        "token_ids": draw_token_ids(jax.random.fold_in(arg_keys[12], 71), 0),
        "token_counts": plant(jax.random.randint(arg_keys[5], (SEQS,), LENGTH // 2, LENGTH + 1), jax.random.fold_in(arg_keys[5], 1), LENGTH // 2, LENGTH).astype(jnp.int32),
        "teacher_out": scatter_about(arg_keys[6], (SEQS, LENGTH, D), 1.0, 6.0, ((0, 4), (1, 8))),
        "out_weight": scatter_about(arg_keys[7], (DI, D), DI ** -0.5, 0.1875, ((0, 32),), jnp.float32),
        "decay_log": draw_decay_log(jax.random.fold_in(arg_keys[12], 71), 0),
        "step_bias": jnp.clip(jax.random.uniform(arg_keys[9], (H,), jnp.float32, -5.0, -3.0), -5.0, -3.0),
        "skip_gain": jnp.clip(jax.random.uniform(arg_keys[10], (H,), jnp.float32, 0.5, 1.5), 0.5, 1.5),
        "norm_gain": jnp.clip(1.0 + 0.1 * jax.random.normal(arg_keys[11], (DI,), jnp.float32), 0.5, 1.5),
    }


norm_floor = 1.0
clip_limit = 1.0
learn_rate = 8.0
highest = lax.Precision.HIGHEST
masked_low = -10000.0

def step_sizes(decay_log, step_bias, step_raw):
    step_width = jax.nn.softplus(step_raw + step_bias[None, :])
    decay_sum = jnp.cumsum(step_width * (-jnp.exp(decay_log))[None, :], axis=0)
    return (step_width, decay_sum)

def mix_block(decay_log, step_bias, skip_gain, norm_gain, state_in, head_inputs, gate_inputs, b_proj, c_proj, step_raw, segment):
    positions = head_inputs.shape[0]
    head_count = decay_log.shape[0]
    step_width, decay_sum = step_sizes(decay_log, step_bias, step_raw)
    inputs_f = head_inputs.astype(jnp.float32).reshape(positions, head_count, -1)
    scaled = inputs_f * step_width[:, :, None]
    scores = jnp.dot(c_proj, b_proj.T, preferred_element_type=jnp.float32)
    position = jnp.arange(positions)
    allowed = (segment[:, None] == segment[None, :]) & (position[:, None] >= position[None, :])

    def one_head(head_data):
        head_sum, head_scaled = head_data
        spread = head_sum[:, None] - head_sum[None, :]
        decay_grid = jnp.exp(jnp.where(allowed, spread, masked_low))
        return jnp.dot(decay_grid * scores, head_scaled, precision=highest)
    intra_sum = jnp.transpose(lax.map(one_head, (decay_sum.T, jnp.transpose(scaled, (1, 0, 2)))), (1, 0, 2))
    entry_decay = jnp.exp(decay_sum) * (segment == 0)[:, None]
    carried = jnp.einsum('in,hpn->ihp', c_proj.astype(jnp.float32), state_in, precision=highest) * entry_decay[:, :, None]
    mixed_out = intra_sum + carried + skip_gain[None, :, None] * inputs_f
    gated = mixed_out.reshape(positions, -1) * jax.nn.silu(gate_inputs.astype(jnp.float32))
    mean_square = lax.optimization_barrier(jnp.mean(gated * gated, axis=1, keepdims=True))
    return gated * norm_gain[None, :] * lax.rsqrt(mean_square + norm_floor)

def state_block(decay_log, step_bias, head_inputs, b_proj, step_raw, segment):
    positions = head_inputs.shape[0]
    head_count = decay_log.shape[0]
    step_width, decay_sum = step_sizes(decay_log, step_bias, step_raw)
    final_sum = decay_sum[-1]
    same_doc = (segment == segment[-1])[:, None]
    tail_decay = jnp.exp(jnp.where(same_doc, final_sum[None, :] - decay_sum, masked_low))
    inputs_f = head_inputs.astype(jnp.float32).reshape(positions, head_count, -1)
    weighted = inputs_f * (step_width * tail_decay)[:, :, None]
    state_out = jnp.einsum('jhp,jn->hpn', weighted, b_proj.astype(jnp.float32), precision=highest)
    carry_out = jnp.exp(final_sum) * (segment[-1] == 0)
    return (carry_out, state_out)

def kahan_total(partials):

    def add_one(running, element):
        summed_up, correction = running
        adjusted = element - correction
        new_total = summed_up + adjusted
        correction = new_total - summed_up - adjusted
        return ((new_total, correction), None)
    (summed_up, correction), _ = lax.scan(add_one, (jnp.zeros((), jnp.float32), jnp.zeros((), jnp.float32)), partials)
    return summed_up

def reference(head_inputs, gate_inputs, state_proj, time_steps, token_ids, token_counts, teacher_out, out_weight, decay_log, step_bias, skip_gain, norm_gain):
    seq_count, length, inner_width = head_inputs.shape
    state_size = state_proj.shape[2] // 2
    model_width = teacher_out.shape[2]
    blocks = N_SEQ
    block_len = length // blocks
    head_count = decay_log.shape[0]
    head_size = inner_width // head_count

    def split_blocks(array):
        return array.reshape((seq_count, blocks, block_len) + array.shape[2:])
    starts = (token_ids == 0).astype(jnp.int32)
    segments = jnp.cumsum(split_blocks(starts), axis=2).astype(jnp.int32)
    position = jnp.arange(length).astype(jnp.int32)
    scored_all = (position[None, :] < token_counts[:, None]).astype(jnp.float32)
    total_count = jnp.sum(token_counts).astype(jnp.float32)
    pieces = (split_blocks(head_inputs), split_blocks(gate_inputs), split_blocks(state_proj), split_blocks(time_steps), segments)
    losses = []
    for step_index in range(STEPS):
        weight_b = out_weight.astype(jnp.bfloat16)
        params = (decay_log, step_bias, skip_gain, norm_gain)

        def one_sequence(running, seq_data):
            sequence, target_s, scored_s = seq_data

            def forward(params_in):

                def per_block(state_in, block_data):
                    inputs_b, gates_b, proj_b, raw_b, seg_b = block_data
                    normed_blk = mix_block(params_in[0], params_in[1], params_in[2], params_in[3], state_in, inputs_b, gates_b, proj_b[:, :state_size], proj_b[:, state_size:], raw_b, seg_b)
                    carry_out, state_out = state_block(params_in[0], params_in[1], inputs_b, proj_b[:, :state_size], raw_b, seg_b)
                    return (carry_out[:, None, None] * state_in + state_out, normed_blk)
                start_state = jnp.zeros((head_count, head_size, state_size), jnp.float32)
                _, normed_seq = lax.scan(jax.checkpoint(per_block), start_state, sequence)
                return normed_seq
            normed, pull_back = jax.vjp(forward, params)
            normed_b = normed.astype(jnp.bfloat16).reshape(-1, inner_width)
            output = jnp.dot(normed_b, weight_b, preferred_element_type=jnp.float32)
            residual = output - target_s.astype(jnp.float32)
            token_loss = lax.optimization_barrier(jnp.sum(residual * residual, axis=1)) * scored_s / model_width
            block_sums = lax.optimization_barrier(jnp.sum(token_loss.reshape(blocks, block_len), axis=1))
            out_grad = (residual * (2.0 / (model_width * total_count)) * scored_s[:, None]).astype(jnp.bfloat16)
            weight_part = jnp.dot(normed_b.T, out_grad, preferred_element_type=jnp.float32)
            normed_grad = jnp.dot(out_grad, weight_b.T, preferred_element_type=jnp.float32).reshape(normed.shape)
            small_part, = pull_back(normed_grad)
            new_running = (running[0] + weight_part, tuple((left + right for left, right in zip(running[1], small_part))))
            return (new_running, block_sums)
        start_running = (jnp.zeros(out_weight.shape, jnp.float32), tuple((jnp.zeros(member.shape, jnp.float32) for member in params)))
        (weight_grad, small_grads), partial_sums = lax.scan(one_sequence, start_running, (pieces, teacher_out, scored_all))
        losses.append(kahan_total(partial_sums.reshape(-1)) / total_count)
        norm_square = jnp.sum(weight_grad * weight_grad) + sum((jnp.sum(member * member) for member in small_grads))
        factor = clip_limit / jnp.maximum(jnp.sqrt(norm_square), clip_limit)
        out_weight = out_weight - learn_rate * factor * weight_grad
        decay_log = decay_log - learn_rate * factor * small_grads[0]
        step_bias = step_bias - learn_rate * factor * small_grads[1]
        skip_gain = skip_gain - learn_rate * factor * small_grads[2]
        norm_gain = norm_gain - learn_rate * factor * small_grads[3]
    return (jnp.stack(losses), out_weight, decay_log, step_bias, skip_gain, norm_gain)
```

```python
import functools

import jax
import jax.numpy as jnp
from jax import lax
from jax.experimental import pallas as pl
from jax.experimental.pallas import tpu as pltpu
from jax.sharding import PartitionSpec as P

STEPS = 2
norm_floor = 1.0
clip_limit = 1.0
learn_rate = 8.0
log2e = 1.4426950408889634
f32 = jnp.float32
bf16 = jnp.bfloat16
LANES = 128
VMEM = pl.BlockSpec(memory_space=pltpu.VMEM)
SMEM = pl.BlockSpec(memory_space=pltpu.SMEM)
MESH = pl.DeviceIdType.MESH
LIMIT = 60 * 1024 * 1024


def dot(a, b):
    return jnp.dot(a, b, preferred_element_type=f32)


def contract(a, b, da, db):
    return lax.dot_general(a, b, (((da,), (db,)), ((), ())), preferred_element_type=f32)


def iota(shape, axis):
    return lax.broadcasted_iota(jnp.int32, shape, axis)


def fold(a):
    rows, width = a.shape
    return jnp.sum(a.reshape(rows // 8, 8, width), axis=0)


def total(a):
    return jnp.sum(a, axis=0, keepdims=True)


def lane_total(a):
    return jnp.sum(a, axis=1, keepdims=True)


def flat(a):
    k, rows, width = a.shape
    if rows % 16 == 0 or a.dtype == f32:
        return a.reshape(k * rows, width)
    return a.astype(f32).reshape(k * rows, width).astype(a.dtype)


def each(n, body, first=0):
    if n - first <= 3:
        for t in range(first, n):
            body(t)
        return

    def one(t, _):
        body(t)
        return 0

    lax.fori_loop(first, n, one, 0)


def remote(source, target, send, recv, peer):
    return pltpu.make_async_remote_copy(
        src_ref=source,
        dst_ref=target,
        send_sem=send,
        recv_sem=recv,
        device_id=peer,
        device_id_type=MESH,
    )


class Refs:
    def __init__(self, names, refs):
        self.__dict__.update(zip(names, refs))


class Spot:
    def __init__(self, n_dp, n_seq):
        self.n_dp, self.n_seq, self.n = n_dp, n_seq, n_dp * n_seq
        self.cores = 2 if n_dp % 2 == 0 else 1
        self.ys = n_dp // self.cores
        self.highs = 4 if n_seq % 4 == 0 else n_seq
        self.lows = n_seq // self.highs
        self.dp, self.seq = lax.axis_index("dp"), lax.axis_index("seq")
        self.y, self.core = self.dp // self.cores, self.dp % self.cores
        self.high, self.low = self.seq // self.lows, self.seq % self.lows
        self.me = self.dp * n_seq + self.seq
        y = (self.ys, self.y, self.y_peer)
        x = (self.lows, self.low, self.low_peer)
        self.orders = [(y, x), (x, y)]

    def core_peer(self, t):
        return (self.y * self.cores + (self.core + t) % self.cores, self.seq)

    def y_peer(self, t):
        return (((self.y + t) % self.ys) * self.cores + self.core, self.seq)

    def low_peer(self, t):
        return (self.dp, self.high * self.lows + (self.low + t) % self.lows)

    def high_peer(self, t):
        return (self.dp, ((self.high + t) % self.highs) * self.lows + self.low)

    def seq_peer(self, t):
        return (self.dp, (self.seq + t) % self.n_seq)

    def any_peer(self, t):
        to = (self.me + t) % self.n
        return (to // self.n_seq, to % self.n_seq)

    def plane_peer(self, t):
        to = (self.dp * self.lows + self.low + t) % (self.n_dp * self.lows)
        return (to // self.lows, self.high * self.lows + to % self.lows)

    def split(self, k, first, second):
        return (first, second) if k == 0 else (second, first)

    def seq_at(self, high, low):
        return high * self.lows + low

    def chunk(self, y, seq):
        return (y * self.cores + self.core) * self.n_seq + seq

    def greet(self):
        barrier = pltpu.get_barrier_semaphore()
        each(
            self.n,
            lambda t: pl.semaphore_signal(
                barrier, inc=1, device_id=self.any_peer(t), device_id_type=MESH
            ),
            1,
        )

    def meet(self):
        pl.semaphore_wait(pltpu.get_barrier_semaphore(), self.n - 1)


def to_column(row, k, heads):
    sub, lane = iota((heads, LANES), 0), iota((heads, LANES), 1)
    return lane_total(jnp.where(lane == k * heads + sub, row, 0.0))


def to_row(column, k):
    heads = column.shape[0]
    sub, lane = iota((heads, LANES), 0), iota((heads, LANES), 1)
    return total(jnp.where(lane == k * heads + sub, column, 0.0))


def accumulate(a, upper, axis):
    rows = a.shape[0]
    high = a.astype(bf16)
    rest = a - high.astype(f32)
    mid = rest.astype(bf16)
    low = (rest - mid.astype(f32)).astype(bf16)
    out = contract(jnp.concatenate([high, mid, low], axis=0), upper, 1, axis)
    return out[:rows] + out[rows : 2 * rows] + out[2 * rows :]


class Gather:
    def __init__(self, at, r):
        self.at, self.r = at, r

    def push(self, k, chunk, send, peer):
        r = self.r
        return remote(r.full.at[k, chunk], r.full.at[k, chunk], send, r.w_recv.at[k, chunk], peer)

    def arrived(self, k, chunk):
        self.push(k, chunk, self.r.wz_send.at[k, 0], self.at.core_peer(1)).wait_recv()

    def high_edge(self, k, t):
        return self.push(k, self.at.me, self.r.wz_send.at[k, t], self.at.high_peer(t))

    def inner_edge(self, k, t, high):
        at = self.at
        (_, _, _), (_, _, peer) = at.orders[k]
        chunk = at.chunk(at.y, at.seq_at(high, at.low))
        return self.push(k, chunk, self.r.wi_send.at[k, t * at.highs + high], peer(t))

    def outer_edge(self, k, t, second, high):
        at = self.at
        (_, first, peer), (count, _, _) = at.orders[k]
        y, low = at.split(k, first, second)
        chunk = at.chunk(y, at.seq_at(high, low))
        send = self.r.wo_send.at[k, (t * count + second) * at.highs + high]
        return self.push(k, chunk, send, peer(t))

    def core_edge(self, k, t, y, seq):
        at = self.at
        send = self.r.wc_send.at[k, (t * at.ys + y) * at.n_seq + seq]
        return self.push(k, at.chunk(y, seq), send, at.core_peer(t))

    def onward(self, k, y, low, high, to_inner, to_outer):
        at = self.at
        (outers, _, _), (inners, _, _) = at.orders[k]
        second = low if k == 0 else y
        if to_inner:
            each(inners, lambda t: self.inner_edge(k, t, high).start(), 1)
        if to_outer:
            each(outers, lambda t: self.outer_edge(k, t, second, high).start(), 1)
        each(at.cores, lambda t: self.core_edge(k, t, y, at.seq_at(high, low)).start(), 1)

    def start(self):
        at = self.at
        for k in range(2):
            each(at.highs, lambda t: self.high_edge(k, t).start(), 1)
        for k in range(2):
            self.onward(k, at.y, at.low, at.high, True, True)

    def from_high(self):
        at = self.at

        def one(t):
            high = (at.high + at.highs - t) % at.highs
            for k in range(2):
                self.arrived(k, at.chunk(at.y, at.seq_at(high, at.low)))
                self.onward(k, at.y, at.low, high, True, True)

        each(at.highs, one, 1)

    def from_inner(self):
        at = self.at

        def pick(k, t, u):
            (_, first, _), (count, second, _) = at.orders[k]
            y, low = at.split(k, first, (second + count - t) % count)
            high = (at.high + at.highs - u) % at.highs
            self.arrived(k, at.chunk(y, at.seq_at(high, low)))
            self.onward(k, y, low, high, False, True)

        def both(u):
            for k in range(2):
                each(at.orders[k][1][0], lambda t: pick(k, t, u), 1)

        each(at.highs, both)

    def from_outer(self):
        at = self.at

        def pick(k, t, v):
            (count, first, _), (inners, second, _) = at.orders[k]
            other = (second + v // at.highs) % inners
            high = (at.high + v) % at.highs
            y, low = at.split(k, (first + count - t) % count, other)
            self.arrived(k, at.chunk(y, at.seq_at(high, low)))
            self.onward(k, y, low, high, False, False)

        for k in range(2):
            (count, _, _), (inners, _, _) = at.orders[k]
            each(count, lambda t: each(inners * at.highs, lambda v: pick(k, t, v)), 1)

    def from_core(self):
        at = self.at

        def one(t, v):
            core = (at.core + t) % at.cores
            chunk = ((v // at.n_seq) * at.cores + core) * at.n_seq + v % at.n_seq
            for k in range(2):
                self.arrived(k, chunk)

        each(at.cores, lambda t: each(at.ys * at.n_seq, lambda v: one(t, v)), 1)

    def drain(self):
        at = self.at
        for k in range(2):
            (outers, _, _), (inners, _, _) = at.orders[k]
            each(at.highs, lambda t: self.high_edge(k, t).wait_send(), 1)
            each(
                inners,
                lambda t: each(at.highs, lambda u: self.inner_edge(k, t, u).wait_send()),
                1,
            )
            each(
                outers,
                lambda t: each(
                    inners * at.highs,
                    lambda v: self.outer_edge(k, t, v // at.highs, v % at.highs).wait_send(),
                ),
                1,
            )
            each(
                at.cores,
                lambda t: each(
                    at.ys * at.n_seq,
                    lambda v: self.core_edge(k, t, v // at.n_seq, v % at.n_seq).wait_send(),
                ),
                1,
            )


class Scatter:
    def __init__(self, at, r):
        self.at, self.r = at, r

    def core_edge(self, k, t, y):
        at, r = self.at, self.r
        dp = y * at.cores + (at.core + t) % at.cores
        slot = t * at.ys + y
        return remote(
            r.grad.at[k, pl.ds(dp * at.n_seq, at.n_seq)], r.from_core.at[k, slot],
            r.gc_send.at[k, slot], r.gc_recv.at[k, slot], at.core_peer(t),
        )

    def first_edge(self, k, t, a):
        at, r = self.at, self.r
        (_, _, peer), (count, _, _) = at.orders[k]
        slot = t * count + a
        return remote(
            r.staged1.at[k, slot], r.from1.at[k, slot],
            r.g1_send.at[k, slot], r.g1_recv.at[k, slot], peer(t),
        )

    def second_edge(self, k, t):
        at, r = self.at, self.r
        peer = at.orders[k][1][2]
        return remote(
            r.staged2.at[k, t], r.from2.at[k, t], r.g2_send.at[k, t], r.g2_recv.at[k, t], peer(t)
        )

    def high_edge(self, k, t):
        at, r = self.at, self.r
        return remote(
            r.staged3.at[k, t], r.from3.at[k, t],
            r.g3_send.at[k, t], r.g3_recv.at[k, t], at.high_peer(t),
        )

    def chip_sum(self, k, first, second, high):
        at, r = self.at, self.r
        y, low = at.split(k, first, second)
        seq = at.seq_at(high, low)
        acc = r.grad[k, at.chunk(y, seq)].astype(f32)
        for t in range(1, at.cores):
            acc = acc + r.from_core[k, t * at.ys + y, seq].astype(f32)
        return acc

    def first_sum(self, k, second, high):
        at, r = self.at, self.r
        (firsts, first, _), (count, _, _) = at.orders[k]
        acc = self.chip_sum(k, first, second, high)
        for t in range(1, firsts):
            acc = acc + r.from1[k, t * count + second, high].astype(f32)
        return acc

    def second_sum(self, k, high):
        at, r = self.at, self.r
        _, (count, second, _) = at.orders[k]
        acc = self.first_sum(k, second, high)
        for t in range(1, count):
            acc = acc + r.from2[k, t, high].astype(f32)
        return acc

    def to_first(self):
        at, r = self.at, self.r
        for t in range(1, at.cores):
            for k in range(2):
                each(at.ys, lambda y: self.core_edge(k, t, y).wait_recv())

        def pick(k, t, v):
            (firsts, first, _), (count, second, _) = at.orders[k]
            a = (second + 1 + v) % count

            def one(high):
                acc = self.chip_sum(k, (first + t) % firsts, a, high)
                r.staged1[k, t * count + a, high] = acc.astype(bf16)

            each(at.highs, one)
            self.first_edge(k, t, a).start()

        top = max(order[1][0] for order in at.orders)
        for v in range(top):
            for k in range(2):
                (firsts, _, _), (count, _, _) = at.orders[k]
                if v < count:
                    each(firsts, lambda t: pick(k, t, v), 1)

    def to_second(self):
        at, r = self.at, self.r

        def pick(k, t):
            (firsts, _, _), (count, second, _) = at.orders[k]
            a = (second + t) % count
            each(firsts, lambda u: self.first_edge(k, u, a).wait_recv(), 1)

            def one(high):
                r.staged2[k, t, high] = self.first_sum(k, a, high).astype(bf16)

            each(at.highs, one)
            self.second_edge(k, t).start()

        for k in range(2):
            each(at.orders[k][1][0], lambda t: pick(k, t), 1)

    def to_high(self):
        at, r = self.at, self.r
        for k in range(2):
            (firsts, _, _), (count, second, _) = at.orders[k]
            each(firsts, lambda u: self.first_edge(k, u, second).wait_recv(), 1)
            each(count, lambda t: self.second_edge(k, t).wait_recv(), 1)

            def one(t):
                acc = self.second_sum(k, (at.high + t) % at.highs)
                r.staged3[k, t] = acc.astype(bf16)
                self.high_edge(k, t).start()

            each(at.highs, one, 1)

    def finish(self):
        at, r = self.at, self.r
        half = r.acc.shape[1] // 2
        square = None
        for k in range(2):
            acc = self.second_sum(k, at.high)
            each(at.highs, lambda t: self.high_edge(k, t).wait_recv(), 1)
            for t in range(1, at.highs):
                acc = acc + r.from3[k, t].astype(f32)
            r.acc[:, k * half : (k + 1) * half] = acc
            part = fold(acc * acc)
            square = part if square is None else square + part
        return lane_total(total(square))

    def drain(self):
        at = self.at
        for k in range(2):
            (firsts, _, _), (count, _, _) = at.orders[k]
            for t in range(1, at.cores):
                each(at.ys, lambda y: self.core_edge(k, t, y).wait_send())
            each(
                firsts,
                lambda t: each(count, lambda a: self.first_edge(k, t, a).wait_send()),
                1,
            )
            each(count, lambda t: self.second_edge(k, t).wait_send(), 1)
            each(at.highs, lambda t: self.high_edge(k, t).wait_send(), 1)


class Exchange:
    def __init__(self, at, state, landed, ready, entering, sems):
        self.at, self.state, self.landed, self.ready, self.entering = (
            at, state, landed, ready, entering,
        )
        self.s_send, self.s_recv, self.r_send, self.r_recv = sems

    def back(self, t):
        return (self.at.seq + self.at.n_seq - t) % self.at.n_seq

    def first(self, t):
        p = (self.at.seq + t) % self.at.n_seq
        return remote(
            self.state.at[p], self.landed.at[self.at.seq],
            self.s_send.at[t], self.s_recv.at[t], self.at.seq_peer(t),
        )

    def first_in(self, t):
        p = self.back(t)
        return remote(
            self.state.at[p], self.landed.at[p],
            self.s_send.at[t], self.s_recv.at[t], self.at.seq_peer(t),
        )

    def second(self, t):
        p = (self.at.seq + t) % self.at.n_seq
        return remote(
            self.ready.at[p], self.entering.at[self.at.seq],
            self.r_send.at[t], self.r_recv.at[t], self.at.seq_peer(t),
        )

    def second_in(self, t):
        p = self.back(t)
        return remote(
            self.ready.at[p], self.entering.at[p],
            self.r_send.at[t], self.r_recv.at[t], self.at.seq_peer(t),
        )

    def start(self):
        each(self.at.n_seq, lambda t: self.first(t).start(), 1)
        self.landed[self.at.seq] = self.state[self.at.seq]

    def turn(self, carries, size, order):
        mine, n_seq = self.at.seq, self.at.n_seq
        each(n_seq, lambda t: self.first_in(t).wait_recv(), 1)
        piece, ns = self.state.shape[1:]
        per = piece // size
        for q in range(per):
            rows = slice(q * size, (q + 1) * size)
            running = jnp.zeros((size, ns), f32)
            for n, d in enumerate(order):
                self.ready[d, rows, :] = running.astype(bf16)
                if n < n_seq - 1:
                    kept = carries[d, pl.ds(mine * per + q, 1), :]
                    running = kept * running + self.landed[d, rows, :].astype(f32)
        each(n_seq, lambda t: self.second(t).start(), 1)
        self.entering[mine] = self.ready[mine]

    def finish(self):
        each(self.at.n_seq, lambda t: self.second_in(t).wait_recv(), 1)

    def drain(self):
        each(self.at.n_seq, lambda t: self.first(t).wait_send(), 1)
        each(self.at.n_seq, lambda t: self.second(t).wait_send(), 1)


def train_kernel(n_dp, n_seq, names, *refs):
    r = Refs(names, refs)
    at = Spot(n_dp, n_seq)
    inner, tokens = r.xt.shape
    heads = r.decay.shape[1]
    size = inner // heads
    ns = r.proj.shape[1] // 2
    share, model = r.rows.shape
    half = model // 2
    g = inner // LANES
    blocks = tokens // LANES
    head_rows = [slice(h * size, (h + 1) * size) for h in range(heads)]
    gather, scatter = Gather(at, r), Scatter(at, r)
    fore = Exchange(
        at, r.state, r.landed, r.ready, r.entering, (r.s_send, r.s_recv, r.r_send, r.r_recv)
    )
    rear = Exchange(
        at, r.b_state, r.b_landed, r.b_ready, r.leaving,
        (r.bs_send, r.bs_recv, r.br_send, r.br_recv),
    )
    b, c = slice(0, ns), slice(ns, 2 * ns)

    def wide(column):
        return jnp.concatenate([column] * blocks, axis=1)

    def lead(t):
        return remote(
            r.carries.at[at.seq], r.carries.at[at.seq],
            r.c_send.at[t], r.c_recv.at[t], at.seq_peer(t),
        )

    def lead_in(t):
        p = (at.seq + n_seq - t) % n_seq
        return remote(
            r.carries.at[p], r.carries.at[p], r.c_send.at[t], r.c_recv.at[t], at.seq_peer(t)
        )

    plane = n_dp * at.lows
    place = at.dp * at.lows + at.low

    def plane_edge(t, slot):
        return remote(
            r.gain_a.at[place], r.gain_a.at[slot],
            r.pa_send.at[t], r.pa_recv.at[t], at.plane_peer(t),
        )

    def line_edge(t, slot):
        return remote(
            r.gain_b.at[at.high], r.gain_b.at[slot],
            r.pb_send.at[t], r.pb_recv.at[t], at.high_peer(t),
        )

    at.greet()
    r.held[...] = r.rows[...]
    for k, ref in enumerate((r.decay, r.bias, r.skip)):
        sub, lane = iota((heads, heads), 0), iota((heads, heads), 1)
        own = lane_total(jnp.where(sub == lane, ref[...], 0.0))
        row = to_row(own, k)
        packed = row if k == 0 else packed + row
    r.params[...] = packed
    r.gain_now[...] = r.gain[...]
    r.upper[...] = (iota((tokens, tokens), 0) <= iota((tokens, tokens), 1)).astype(bf16)
    for k in range(g):
        cols = slice(k * LANES, (k + 1) * LANES)
        r.xt[cols, :] = r.x[:, cols].astype(f32).T
    stop = jnp.where(r.ids[...] == 0, 1.0, 0.0)
    r.seg[...] = dot(jnp.broadcast_to(stop, (16, tokens)).astype(bf16), r.upper[...])

    def prepare():
        seg_c = r.seg[...].T[:, 0:1]
        raw = contract(r.proj[:, b], r.proj[:, c], 1, 1)
        open_to = (seg_c == r.seg[0:1, :]) & (
            iota((tokens, tokens), 0) <= iota((tokens, tokens), 1)
        )
        r.score[...] = jnp.where(open_to, raw, 0.0)
        for k in range(g):
            cols = slice(k * LANES, (k + 1) * LANES)
            zt = r.z[:, cols].astype(f32).T
            r.gate[cols, :] = zt * jax.nn.sigmoid(zt)

    def forward_head(h):
        rows = head_rows[h]
        for jb in range(blocks):
            js = slice(jb * LANES, (jb + 1) * LANES)
            left = r.sums_c[js, h : h + 1]
            for ib in range(jb, blocks):
                cs = slice(ib * LANES, (ib + 1) * LANES)
                gap = r.sums[h : h + 1, cs] - left
                if ib == jb:
                    gap = jnp.minimum(gap, 0.0)
                r.grid[h, js, cs] = (jnp.exp2(gap) * r.score[js, cs]).astype(bf16)
        for ib in range(blocks):
            end = (ib + 1) * LANES
            cs = slice(ib * LANES, end)
            r.mixed[rows, cs] = dot(r.scaled[rows, :end], r.grid[h, :end, cs])

    def backward_head(h):
        rows = head_rows[h]
        for jb in range(blocks):
            at_j = jb * LANES
            js = slice(at_j, at_j + LANES)
            part = contract(r.slope[rows, at_j:], r.grid[h, js, at_j:], 1, 1)
            r.col_dot[h : h + 1, js] = total(part * r.xt[rows, js])

    def step(s, _):
        for k in range(2):
            r.full[k, at.me] = r.held[:, k * half : (k + 1) * half].astype(bf16)

        @pl.when(s == 0)
        def _():
            at.meet()

        gather.start()

        packed = r.params[...]
        rate = -jnp.exp(jnp.broadcast_to(to_column(packed, 0, heads), (heads, tokens)))
        bias = jnp.broadcast_to(to_column(packed, 1, heads), (heads, tokens))
        w = jax.nn.softplus(r.raw_t[...] + bias)
        sums = accumulate(w * (rate * log2e), r.upper[...], 0)
        seg = r.seg[...][:heads]
        final = sums[:, tokens - 1 : tokens]
        last = seg[:, tokens - 1 : tokens]
        tail = jnp.where(seg == last, jnp.exp2(final - sums), 0.0)
        r.rate[...] = rate
        r.bias_w[...] = bias
        r.width[...] = w
        r.sums[...] = sums
        r.tail[...] = tail
        r.ending[...] = w * tail
        r.entry[...] = jnp.where(seg == 0.0, jnp.exp2(sums), 0.0)
        r.carries[at.seq] = jnp.broadcast_to(
            jnp.where(last == 0.0, jnp.exp2(final), 0.0), (heads, LANES)
        )
        for h in range(heads):
            rows = head_rows[h]
            r.slope[rows, :] = (r.xt[rows, :] * r.ending[h : h + 1, :]).astype(bf16)
        ended = dot(r.slope[...], r.proj[:, b])
        r.state[...] = ended.reshape(r.state.shape).astype(bf16)
        each(n_seq, lambda t: lead(t).start(), 1)
        fore.start()

        r.sums_c[...] = sums.T
        for h in range(heads):
            rows = head_rows[h]
            r.scaled[rows, :] = (r.xt[rows, :] * r.width[h : h + 1, :]).astype(bf16)

        @pl.when(s == 0)
        def _():
            prepare()

        gather.from_high()
        for k in range(g):
            row = jnp.broadcast_to(r.gain_now[k : k + 1, :], (LANES, LANES))
            r.gain_w[k * LANES : (k + 1) * LANES, :] = row.T
        cut = heads // 4
        for h in range(cut):
            forward_head(h)
        gather.from_inner()
        each(n_seq, lambda t: lead_in(t).wait_recv(), 1)
        fore.turn(r.carries, size, list(range(n_seq)))
        for h in range(cut, 3 * cut):
            forward_head(h)
        gather.from_outer()
        for h in range(3 * cut, heads):
            forward_head(h)
        fore.finish()

        passed = contract(flat(r.entering[...]), r.proj[:, c], 1, 1)
        skip = jnp.broadcast_to(to_column(packed, 2, heads), (heads, tokens))
        r.skip_w[...] = skip
        power = jnp.zeros((8, tokens), f32)
        for h in range(heads):
            rows = head_rows[h]
            y = r.mixed[rows, :] + passed[rows, :] * r.entry[h : h + 1, :]
            r.mixed[rows, :] = y
            gated = (y + r.skip_w[h : h + 1, :] * r.xt[rows, :]) * r.gate[rows, :]
            r.gated[rows, :] = gated
            power = power + fold(gated * gated)
        root = lax.rsqrt(total(power) * (1.0 / inner) + norm_floor)
        r.root[...] = jnp.broadcast_to(root, r.root.shape)
        for k in range(g):
            rows = slice(k * LANES, (k + 1) * LANES)
            normed = r.gated[rows, :] * wide(r.gain_w[rows, :]) * r.root[0:1, :]
            r.normed[rows, :] = normed.astype(bf16)
            r.normed_n[:, rows] = normed.T.astype(bf16)

        gather.from_core()
        for k in range(2):
            r.residual[:, k * half : (k + 1) * half] = dot(r.normed_n[...], flat(r.full[k]))
        count = r.counts[0]
        for k in range(1, n_dp):
            count = count + r.counts[k]
        share_of = 1.0 / (model * count.astype(f32))
        limit = r.counts[at.dp] - at.seq * tokens
        lost = jnp.zeros((8, model), f32)
        step_rows = 32
        for q in range(tokens // step_rows):
            rows = slice(q * step_rows, (q + 1) * step_rows)
            scored = iota((step_rows, model), 0) + q * step_rows < limit
            gap = jnp.where(scored, r.residual[rows, :] - r.target[rows, :].astype(f32), 0.0)
            lost = lost + fold(gap * gap)
            r.og[rows, :] = (gap * (2.0 * share_of)).astype(bf16)
        loss = lane_total(total(lost)) * share_of

        def weight_part(t, y):
            dp = y * at.cores + (at.core + t) % at.cores
            width = n_seq * share
            left = r.normed[pl.ds(pl.multiple_of(dp * width, width), width), :]
            for k in range(2):
                out = dot(left, r.og[:, k * half : (k + 1) * half])
                r.grad[k, pl.ds(dp * n_seq, n_seq)] = out.reshape(n_seq, share, half).astype(bf16)
                if t > 0:
                    scatter.core_edge(k, t, y).start()

        for t in range(1, at.cores):
            for u in range(at.ys):
                weight_part(t, (at.y + 1 + u) % at.ys)
        r.ng[...] = contract(flat(r.full[0]), r.og[:, :half], 1, 1)
        r.ng[...] += contract(flat(r.full[1]), r.og[:, half:], 1, 1)
        inward = jnp.zeros((8, tokens), f32)
        for h in range(heads):
            rows = head_rows[h]
            lifted = r.ng[rows, :] * r.gated[rows, :]
            inward = inward + fold(lifted * wide(r.gain_w[rows, :]))
            lifted = lifted * r.root[0:1, :]
            part = lifted[:, :LANES]
            for k in range(1, blocks):
                part = part + lifted[:, k * LANES : (k + 1) * LANES]
            r.gain_part[rows, :] = part
        root = r.root[0:1, :]
        inward = total(inward) * (root * root * root * (1.0 / inner))
        r.inward[...] = jnp.broadcast_to(inward, r.inward.shape)
        for h in range(heads):
            rows = head_rows[h]
            dy = r.ng[rows, :] * wide(r.gain_w[rows, :]) * r.root[0:1, :]
            dy = (dy - r.gated[rows, :] * r.inward[0:1, :]) * r.gate[rows, :]
            r.row_dot[h : h + 1, :] = total(dy * r.mixed[rows, :])
            r.skip_dot[h : h + 1, :] = total(dy * r.xt[rows, :])
            r.slope[rows, :] = dy.astype(bf16)
            r.scaled[rows, :] = (dy * r.entry[h : h + 1, :]).astype(bf16)
        pulled = dot(r.scaled[...], r.proj[:, c])
        r.b_state[...] = pulled.reshape(r.b_state.shape).astype(bf16)
        rear.start()
        for u in range(at.ys):
            weight_part(0, (at.y + 1 + u) % at.ys)
        for k in range(g):
            rows = slice(k * LANES, (k + 1) * LANES)
            r.gain_a[place, k : k + 1, :] = total(r.gain_part[rows, :].T)
        each(plane, lambda t: plane_edge(t, place).start(), 1)
        scatter.to_first()
        for h in range(cut):
            backward_head(h)
        rear.turn(r.carries, size, list(reversed(range(n_seq))))
        for h in range(cut, 3 * cut):
            backward_head(h)
        scatter.to_second()
        for h in range(3 * cut, heads):
            backward_head(h)
        each(plane, lambda t: plane_edge(t, (place + plane - t) % plane).wait_recv(), 1)
        gain_sum = r.gain_a[0]
        for k in range(1, plane):
            gain_sum = gain_sum + r.gain_a[k]
        r.gain_b[at.high] = gain_sum
        each(at.highs, lambda t: line_edge(t, at.high).start(), 1)
        scatter.to_high()
        gather.drain()
        rear.finish()

        after = flat(r.leaving[...])
        moved = contract(after, r.proj[:, b], 1, 1)
        for h in range(heads):
            rows = head_rows[h]
            r.pulled[h : h + 1, :] = total(moved[rows, :] * r.xt[rows, :])
        piece = r.leaving.shape[1]
        for h in range(heads):
            p, q = (h * size) // piece, (h * size) % piece
            own = r.leaving[p, q : q + size, :].astype(f32)
            own = own * r.entering[p, q : q + size, :].astype(f32)
            r.kept[h : h + 1, :] = total(own)
        drawn = r.pulled[...] * r.tail[...]
        w, rate = r.width[...], r.rate[...]
        col = r.col_dot[...] + drawn
        d_final = lane_total(w * drawn) + lane_total(r.kept[...] * r.carries[at.seq])
        d_rate = accumulate(r.row_dot[...] - w * col, r.upper[...], 1) + d_final
        d_width = (col + rate * d_rate) * jax.nn.sigmoid(r.raw_t[...] + r.bias_w[...])
        message = (
            to_row(lane_total(rate * d_rate * w), 0)
            + to_row(lane_total(d_width), 1)
            + to_row(lane_total(r.skip_dot[...]), 2)
        )
        square = scatter.finish()
        lane = iota((1, LANES), 1)
        message = message + jnp.where(lane == 3 * heads, loss, 0.0)
        message = message + jnp.where(lane == 3 * heads + 1, square, 0.0)
        r.inbox[s, at.me] = message

        def news(t, slot):
            return remote(
                r.inbox.at[s, at.me], r.inbox.at[s, slot],
                r.n_send.at[t], r.n_recv.at[t], at.any_peer(t),
            )

        each(at.n, lambda t: news(t, at.me).start(), 1)
        each(at.highs, lambda t: line_edge(t, (at.high + at.highs - t) % at.highs).wait_recv(), 1)
        gain_sum = r.gain_b[0]
        for k in range(1, at.highs):
            gain_sum = gain_sum + r.gain_b[k]
        scatter.drain()
        fore.drain()
        rear.drain()
        each(n_seq, lambda t: lead(t).wait_send(), 1)
        each(plane, lambda t: plane_edge(t, place).wait_send(), 1)
        each(at.highs, lambda t: line_edge(t, at.high).wait_send(), 1)
        each(at.n, lambda t: news(t, (at.me + at.n - t) % at.n).wait_recv(), 1)
        each(at.n, lambda t: news(t, at.me).wait_send(), 1)
        sums = jnp.sum(r.inbox[s], axis=0)
        small = jnp.where(lane < 3 * heads, sums, 0.0)
        norm = lane_total(small * small + total(gain_sum * gain_sum))
        norm = norm + lane_total(jnp.where(lane == 3 * heads + 1, sums, 0.0))
        pace = learn_rate * clip_limit / jnp.maximum(jnp.sqrt(norm), clip_limit)
        r.params[...] = r.params[...] - pace * small
        r.gain_now[...] = r.gain_now[...] - pace * gain_sum
        r.held[...] = r.held[...] - pace * r.acc[...]
        r.out_small[pl.ds(s + 1, 1), :] = jnp.broadcast_to(
            lane_total(jnp.where(lane == 3 * heads, sums, 0.0)), (1, LANES)
        )
        return 0

    lax.fori_loop(0, STEPS, step, 0)
    r.out_small[0:1, :] = r.params[...]
    r.out_gain[...] = r.gain_now[...]
    r.out_rows[...] = r.held[...]


def finish_kernel(rows, small, gain, losses, new_rows, decay, bias, skip, new_gain):
    heads = decay.shape[1]
    new_rows[...] = rows[...]
    new_gain[...] = gain[...]
    for k, ref in enumerate((decay, bias, skip)):
        ref[...] = small[0:1, k * heads : (k + 1) * heads]
    lane = iota((1, LANES), 1)
    both = jnp.where(lane == 0, small[1:2, :], small[2:3, :])
    losses[...] = both[:, :STEPS]


def call(body, outs, args, scratch=(), **extra):
    return pl.pallas_call(
        body,
        out_shape=tuple(jax.ShapeDtypeStruct(*o) for o in outs),
        in_specs=[SMEM if a.ndim == 1 else VMEM for a in args],
        out_specs=tuple([VMEM] * len(outs)),
        scratch_shapes=list(scratch),
        compiler_params=pltpu.CompilerParams(vmem_limit_bytes=LIMIT, **extra),
    )(*args)


def per_device(
    n_dp,
    n_seq,
    head_inputs,
    gate_inputs,
    state_proj,
    time_steps,
    token_ids,
    token_counts,
    teacher_out,
    out_weight,
    decay_log,
    step_bias,
    skip_gain,
    norm_gain,
):
    n = n_dp * n_seq
    x, z, target, raw = head_inputs[0], gate_inputs[0], teacher_out[0], time_steps[0]
    tokens, inner = x.shape
    ns = state_proj.shape[2] // 2
    heads = decay_log.shape[0]
    model = target.shape[1]
    half = model // 2
    share = out_weight.shape[0]
    piece = inner // n_seq
    g = inner // LANES
    cores = 2 if n_dp % 2 == 0 else 1
    ys = n_dp // cores
    highs = 4 if n_seq % 4 == 0 else n_seq
    lows = n_seq // highs
    most = max(ys, lows)
    per_head, tall = ((heads, tokens), f32), (inner, tokens)
    state = ((n_seq, piece, ns), bf16)
    dma = pltpu.SemaphoreType.DMA
    vmem = {
        "xt": (tall, f32),
        "gate": (tall, f32),
        "mixed": (tall, f32),
        "gated": (tall, f32),
        "ng": (tall, f32),
        "scaled": (tall, bf16),
        "slope": (tall, bf16),
        "normed": (tall, bf16),
        "normed_n": ((tokens, inner), bf16),
        "residual": ((tokens, model), f32),
        "og": ((tokens, model), bf16),
        "upper": ((tokens, tokens), bf16),
        "score": ((tokens, tokens), f32),
        "grid": ((heads, tokens, tokens), bf16),
        "seg": ((16, tokens), f32),
        "sums_c": ((tokens, heads), f32),
        "rate": per_head,
        "bias_w": per_head,
        "skip_w": per_head,
        "width": per_head,
        "sums": per_head,
        "tail": per_head,
        "ending": per_head,
        "entry": per_head,
        "row_dot": per_head,
        "skip_dot": per_head,
        "col_dot": per_head,
        "pulled": per_head,
        "kept": ((heads, ns), f32),
        "root": ((8, tokens), f32),
        "inward": ((8, tokens), f32),
        "gain_w": ((inner, LANES), f32),
        "gain_part": ((inner, LANES), f32),
        "gain_now": ((g, LANES), f32),
        "params": ((1, LANES), f32),
        "held": ((share, model), f32),
        "acc": ((share, model), f32),
        "full": ((2, n, share, half), bf16),
        "grad": ((2, n, share, half), bf16),
        "from_core": ((2, cores * ys, n_seq, share, half), bf16),
        "staged1": ((2, most * most, highs, share, half), bf16),
        "from1": ((2, most * most, highs, share, half), bf16),
        "staged2": ((2, most, highs, share, half), bf16),
        "from2": ((2, most, highs, share, half), bf16),
        "staged3": ((2, highs, share, half), bf16),
        "from3": ((2, highs, share, half), bf16),
        "state": state,
        "landed": state,
        "ready": state,
        "entering": state,
        "b_state": state,
        "b_landed": state,
        "b_ready": state,
        "leaving": state,
        "carries": ((n_seq, heads, LANES), f32),
        "gain_a": ((n_dp * lows, g, LANES), f32),
        "gain_b": ((highs, g, LANES), f32),
        "inbox": ((STEPS, n, 1, LANES), f32),
    }
    sems = {
        "w_recv": (2, n),
        "wz_send": (2, highs),
        "wi_send": (2, most * highs),
        "wo_send": (2, most * most * highs),
        "wc_send": (2, cores * ys * n_seq),
        "gc_send": (2, cores * ys),
        "gc_recv": (2, cores * ys),
        "g1_send": (2, most * most),
        "g1_recv": (2, most * most),
        "g2_send": (2, most),
        "g2_recv": (2, most),
        "g3_send": (2, highs),
        "g3_recv": (2, highs),
        "pa_send": (n_dp * lows,),
        "pa_recv": (n_dp * lows,),
        "pb_send": (highs,),
        "pb_recv": (highs,),
        "n_send": (n,),
        "n_recv": (n,),
    }
    for name in ("c", "s", "r", "bs", "br"):
        sems[name + "_send"] = (n_seq,)
        sems[name + "_recv"] = (n_seq,)
    given = {
        "counts": token_counts,
        "decay": decay_log.reshape(1, heads),
        "bias": step_bias.reshape(1, heads),
        "skip": skip_gain.reshape(1, heads),
        "gain": norm_gain.reshape(g, LANES),
        "raw_t": raw.T,
        "ids": token_ids,
        "x": x,
        "z": z,
        "target": target,
        "proj": state_proj[0],
        "rows": out_weight,
    }
    outs = {
        "out_rows": ((share, model), f32),
        "out_small": ((8, LANES), f32),
        "out_gain": ((g, LANES), f32),
    }
    names = [*given, *outs, *vmem, *sems]
    rows, small, gain = call(
        functools.partial(train_kernel, n_dp, n_seq, names),
        outs.values(),
        tuple(given.values()),
        [pltpu.VMEM(*v) for v in vmem.values()] + [dma(v) for v in sems.values()],
        collective_id=0,
        has_side_effects=True,
    )
    losses, rows, decay, bias, skip, gain = call(
        finish_kernel,
        [
            ((1, STEPS), f32),
            ((share, model), f32),
            ((1, heads), f32),
            ((1, heads), f32),
            ((1, heads), f32),
            ((g, LANES), f32),
        ],
        (rows, small, gain),
    )
    return (
        losses.reshape(STEPS),
        rows,
        decay.reshape(heads),
        bias.reshape(heads),
        skip.reshape(heads),
        gain.reshape(inner),
    )


def solution(mesh):
    in_specs = (
        P("dp", "seq", None),
        P("dp", "seq", None),
        P("dp", "seq", None),
        P("dp", "seq", None),
        P("dp", "seq"),
        P(),
        P("dp", "seq", None),
        P(("dp", "seq"), None),
        P(),
        P(),
        P(),
        P(),
    )
    out_specs = (P(), P(("dp", "seq"), None), P(), P(), P(), P())
    return jax.shard_map(
        functools.partial(per_device, mesh.shape["dp"], mesh.shape["seq"]),
        mesh=mesh,
        in_specs=in_specs,
        out_specs=out_specs,
        check_vma=False,
    )
```

```python
import functools

import jax
import jax.numpy as jnp
from jax import lax
from jax.experimental import pallas as pl
from jax.experimental.pallas import tpu as pltpu
from jax.sharding import PartitionSpec as P

STEPS = 2
norm_floor = 1.0
clip_limit = 1.0
learn_rate = 8.0
log2e = 1.4426950408889634
f32 = jnp.float32
bf16 = jnp.bfloat16
LANES = 128
VMEM = pl.BlockSpec(memory_space=pltpu.VMEM)
SMEM = pl.BlockSpec(memory_space=pltpu.SMEM)
MESH = pl.DeviceIdType.MESH
LIMIT = 60 * 1024 * 1024


def dot(a, b):
    return jnp.dot(a, b, preferred_element_type=f32)


def contract(a, b, da, db):
    return lax.dot_general(a, b, (((da,), (db,)), ((), ())), preferred_element_type=f32)


def iota(shape, axis):
    return lax.broadcasted_iota(jnp.int32, shape, axis)


def fold(a):
    rows, width = a.shape
    return jnp.sum(a.reshape(rows // 8, 8, width), axis=0)


def total(a):
    return jnp.sum(a, axis=0, keepdims=True)


def lane_total(a):
    return jnp.sum(a, axis=1, keepdims=True)


def flat(a):
    k, rows, width = a.shape
    if rows % 16 == 0 or a.dtype == f32:
        return a.reshape(k * rows, width)
    return a.astype(f32).reshape(k * rows, width).astype(a.dtype)


def each(n, body, first=0):
    if n - first <= 3:
        for t in range(first, n):
            body(t)
        return

    def one(t, _):
        body(t)
        return 0

    lax.fori_loop(first, n, one, 0)


def remote(source, target, send, recv, peer):
    return pltpu.make_async_remote_copy(
        src_ref=source,
        dst_ref=target,
        send_sem=send,
        recv_sem=recv,
        device_id=peer,
        device_id_type=MESH,
    )


class Refs:
    def __init__(self, names, refs):
        self.__dict__.update(zip(names, refs))


class Spot:
    def __init__(self, n_dp, n_seq):
        self.n_dp, self.n_seq, self.n = n_dp, n_seq, n_dp * n_seq
        self.cores = 2 if n_dp % 2 == 0 else 1
        self.ys = n_dp // self.cores
        self.highs = 4 if n_seq % 4 == 0 else n_seq
        self.lows = n_seq // self.highs
        self.dp, self.seq = lax.axis_index("dp"), lax.axis_index("seq")
        self.y, self.core = self.dp // self.cores, self.dp % self.cores
        self.high, self.low = self.seq // self.lows, self.seq % self.lows
        self.me = self.dp * n_seq + self.seq
        self.group = n_seq // 2
        self.part, self.spot = self.seq // self.group, self.seq % self.group

    def core_peer(self, t):
        return (self.y * self.cores + (self.core + t) % self.cores, self.seq)

    def y_peer(self, t):
        return (((self.y + t) % self.ys) * self.cores + self.core, self.seq)

    def low_peer(self, t):
        return (self.dp, self.high * self.lows + (self.low + t) % self.lows)

    def high_peer(self, t):
        return (self.dp, ((self.high + t) % self.highs) * self.lows + self.low)

    def group_peer(self, t):
        return (self.dp, self.part * self.group + (self.spot + t) % self.group)

    def other_half(self):
        return (self.dp, (self.seq + self.group) % self.n_seq)

    def any_peer(self, t):
        to = (self.me + t) % self.n
        return (to // self.n_seq, to % self.n_seq)

    def plane_peer(self, t):
        to = (self.dp * self.lows + self.low + t) % (self.n_dp * self.lows)
        return (to // self.lows, self.high * self.lows + to % self.lows)

    def chunk(self, y, high, low):
        return (y * self.cores + self.core) * self.n_seq + high * self.lows + low

    def greet(self):
        barrier = pltpu.get_barrier_semaphore()
        each(
            self.n,
            lambda t: pl.semaphore_signal(
                barrier, inc=1, device_id=self.any_peer(t), device_id_type=MESH
            ),
            1,
        )

    def meet(self):
        pl.semaphore_wait(pltpu.get_barrier_semaphore(), self.n - 1)


def to_column(row, k, heads):
    sub, lane = iota((heads, LANES), 0), iota((heads, LANES), 1)
    return lane_total(jnp.where(lane == k * heads + sub, row, 0.0))


def to_row(column, k):
    heads = column.shape[0]
    sub, lane = iota((heads, LANES), 0), iota((heads, LANES), 1)
    return total(jnp.where(lane == k * heads + sub, column, 0.0))


def accumulate(a, upper, axis):
    rows = a.shape[0]
    high = a.astype(bf16)
    rest = a - high.astype(f32)
    mid = rest.astype(bf16)
    low = (rest - mid.astype(f32)).astype(bf16)
    out = contract(jnp.concatenate([high, mid, low], axis=0), upper, 1, axis)
    return out[:rows] + out[rows : 2 * rows] + out[2 * rows :]


class Gather:
    def __init__(self, at, r):
        self.at, self.r = at, r

    def push(self, chunk, send, peer):
        r = self.r
        return remote(r.full.at[chunk], r.full.at[chunk], send, r.w_recv.at[chunk], peer)

    def arrived(self, chunk):
        self.push(chunk, self.r.wz_send.at[0], self.at.core_peer(1)).wait_recv()

    def high_edge(self, t):
        return self.push(self.at.me, self.r.wz_send.at[t], self.at.high_peer(t))

    def low_edge(self, t, high):
        at = self.at
        chunk = at.chunk(at.y, high, at.low)
        return self.push(chunk, self.r.wx_send.at[t * at.highs + high], at.low_peer(t))

    def y_edge(self, t, high, low):
        at = self.at
        send = self.r.wy_send.at[(t * at.highs + high) * at.lows + low]
        return self.push(at.chunk(at.y, high, low), send, at.y_peer(t))

    def core_edge(self, t, y, seq):
        at = self.at
        send = self.r.wc_send.at[(t * at.ys + y) * at.n_seq + seq]
        return self.push((y * at.cores + at.core) * at.n_seq + seq, send, at.core_peer(t))

    def onward(self, y, high, low, to_low, to_y):
        at = self.at
        if to_low:
            each(at.lows, lambda t: self.low_edge(t, high).start(), 1)
        if to_y:
            each(at.ys, lambda t: self.y_edge(t, high, low).start(), 1)
        each(at.cores, lambda t: self.core_edge(t, y, high * at.lows + low).start(), 1)

    def start(self):
        at = self.at
        each(at.highs, lambda t: self.high_edge(t).start(), 1)
        self.onward(at.y, at.high, at.low, True, True)

    def from_high(self):
        at = self.at

        def one(t):
            high = (at.high + at.highs - t) % at.highs
            self.arrived(at.chunk(at.y, high, at.low))
            self.onward(at.y, high, at.low, True, True)

        each(at.highs, one, 1)

    def from_low(self, u):
        at = self.at
        high = (at.high + at.highs - u) % at.highs

        def pick(t):
            low = (at.low + at.lows - t) % at.lows
            self.arrived(at.chunk(at.y, high, low))
            self.onward(at.y, high, low, False, True)

        each(at.lows, pick, 1)

    def from_y(self):
        at = self.at

        def one(t, v):
            y = (at.y + at.ys - t) % at.ys
            high = (at.high + at.highs - v % at.highs) % at.highs
            low = (at.low + v // at.highs) % at.lows
            self.arrived(at.chunk(y, high, low))
            self.onward(y, high, low, False, False)

        each(at.ys, lambda t: each(at.n_seq, lambda v: one(t, v)), 1)

    def from_core(self):
        at = self.at

        def one(t, v):
            core = (at.core + t) % at.cores
            self.arrived(((v // at.n_seq) * at.cores + core) * at.n_seq + v % at.n_seq)

        each(at.cores, lambda t: each(at.ys * at.n_seq, lambda v: one(t, v)), 1)

    def drain(self):
        at = self.at
        each(at.highs, lambda t: self.high_edge(t).wait_send(), 1)
        each(at.lows, lambda t: each(at.highs, lambda u: self.low_edge(t, u).wait_send()), 1)
        each(
            at.ys,
            lambda t: each(
                at.n_seq, lambda v: self.y_edge(t, v // at.lows, v % at.lows).wait_send()
            ),
            1,
        )
        each(
            at.cores,
            lambda t: each(
                at.ys * at.n_seq,
                lambda v: self.core_edge(t, v // at.n_seq, v % at.n_seq).wait_send(),
            ),
            1,
        )


class Scatter:
    def __init__(self, at, r):
        self.at, self.r = at, r

    def core_edge(self, t, y):
        at, r = self.at, self.r
        dp = y * at.cores + (at.core + t) % at.cores
        slot = t * at.ys + y
        return remote(
            r.grad.at[pl.ds(dp * at.n_seq, at.n_seq)], r.from_core.at[slot],
            r.gc_send.at[slot], r.gc_recv.at[slot], at.core_peer(t),
        )

    def y_edge(self, t, high, low):
        at, r = self.at, self.r
        slot = (t * at.highs + high) * at.lows + low
        return remote(
            r.staged1.at[slot], r.from1.at[slot],
            r.g1_send.at[slot], r.g1_recv.at[slot], at.y_peer(t),
        )

    def low_edge(self, t, high):
        at, r = self.at, self.r
        slot = t * at.highs + high
        return remote(
            r.staged2.at[slot], r.from2.at[slot],
            r.g2_send.at[slot], r.g2_recv.at[slot], at.low_peer(t),
        )

    def high_edge(self, t):
        at, r = self.at, self.r
        return remote(
            r.staged3.at[t], r.from3.at[t], r.g3_send.at[t], r.g3_recv.at[t], at.high_peer(t)
        )

    def chip_sum(self, y, high, low):
        at, r = self.at, self.r
        acc = r.grad[at.chunk(y, high, low)].astype(f32)
        for t in range(1, at.cores):
            acc = acc + r.from_core[t * at.ys + y, high * at.lows + low].astype(f32)
        return acc

    def y_sum(self, high, low):
        at, r = self.at, self.r
        acc = self.chip_sum(at.y, high, low)
        for t in range(1, at.ys):
            self.y_edge(t, high, low).wait_recv()
            acc = acc + r.from1[(t * at.highs + high) * at.lows + low].astype(f32)
        return acc

    def low_sum(self, high):
        at, r = self.at, self.r
        acc = self.y_sum(high, at.low)
        for t in range(1, at.lows):
            self.low_edge(t, high).wait_recv()
            acc = acc + r.from2[t * at.highs + high].astype(f32)
        return acc

    def to_y(self):
        at, r = self.at, self.r
        for t in range(1, at.cores):
            each(at.ys, lambda y: self.core_edge(t, y).wait_recv())

        def one(t, v):
            low = (at.low + 1 + v // at.highs) % at.lows
            high = (at.high + 1 + v) % at.highs
            acc = self.chip_sum((at.y + t) % at.ys, high, low)
            r.staged1[(t * at.highs + high) * at.lows + low] = acc.astype(bf16)
            self.y_edge(t, high, low).start()

        each(at.ys, lambda t: each(at.n_seq, lambda v: one(t, v)), 1)

    def to_low(self, u):
        at, r = self.at, self.r
        high = (at.high + 1 + u) % at.highs

        def one(t):
            low = (at.low + t) % at.lows
            r.staged2[t * at.highs + high] = self.y_sum(high, low).astype(bf16)
            self.low_edge(t, high).start()

        each(at.lows, one, 1)

    def to_high(self, t):
        at, r = self.at, self.r
        r.staged3[t] = self.low_sum((at.high + t) % at.highs).astype(bf16)
        self.high_edge(t).start()

    def finish(self):
        at, r = self.at, self.r
        acc = self.low_sum(at.high)
        each(at.highs, lambda t: self.high_edge(t).wait_recv(), 1)
        for t in range(1, at.highs):
            acc = acc + r.from3[t].astype(f32)
        r.acc[...] = acc
        return lane_total(total(fold(acc * acc)))

    def drain(self):
        at = self.at
        for t in range(1, at.cores):
            each(at.ys, lambda y: self.core_edge(t, y).wait_send())
        each(
            at.ys,
            lambda t: each(
                at.n_seq, lambda v: self.y_edge(t, v // at.lows, v % at.lows).wait_send()
            ),
            1,
        )
        each(at.lows, lambda t: each(at.highs, lambda u: self.low_edge(t, u).wait_send()), 1)
        each(at.highs, lambda t: self.high_edge(t).wait_send(), 1)


class Exchange:
    def __init__(self, at, reverse, state, landed, ready, entering, middle, sems):
        self.at, self.reverse = at, reverse
        self.state, self.landed, self.ready, self.entering = state, landed, ready, entering
        self.middle = middle
        self.s_send, self.s_recv, self.r_send, self.r_recv, self.m_send, self.m_recv = sems
        self.leader = 1 if reverse else 0

    def back(self, t):
        return (self.at.spot + self.at.group - t) % self.at.group

    def first(self, t):
        p = (self.at.spot + t) % self.at.group
        return remote(
            self.state.at[p], self.landed.at[self.at.spot],
            self.s_send.at[t], self.s_recv.at[t], self.at.group_peer(t),
        )

    def first_in(self, t):
        p = self.back(t)
        return remote(
            self.state.at[p], self.landed.at[p],
            self.s_send.at[t], self.s_recv.at[t], self.at.group_peer(t),
        )

    def second(self, t):
        p = (self.at.spot + t) % self.at.group
        return remote(
            self.ready.at[p], self.entering.at[self.at.spot],
            self.r_send.at[t], self.r_recv.at[t], self.at.group_peer(t),
        )

    def second_in(self, t):
        p = self.back(t)
        return remote(
            self.ready.at[p], self.entering.at[p],
            self.r_send.at[t], self.r_recv.at[t], self.at.group_peer(t),
        )

    def across(self):
        return remote(
            self.middle.at[0], self.middle.at[1],
            self.m_send.at[0], self.m_recv.at[0], self.at.other_half(),
        )

    def start(self):
        at = self.at
        each(at.group, lambda t: self.first(t).start(), 1)
        self.landed[at.spot] = self.state[at.spot]

    def lead(self, carries, size):
        @pl.when(self.at.part == self.leader)
        def _():
            self.turn(carries, size, True)

    def follow(self, carries, size):
        @pl.when(self.at.part != self.leader)
        def _():
            self.turn(carries, size, False)

    def turn(self, carries, size, leads):
        at = self.at
        mine, group = at.spot, at.group
        each(group, lambda t: self.first_in(t).wait_recv(), 1)
        if not leads:
            self.across().wait_recv()
        piece = self.state.shape[1]
        per = piece // size
        order = list(range(group))
        if self.reverse:
            order.reverse()
        for q in range(per):
            rows = slice(q * size, (q + 1) * size)
            if leads:
                running = jnp.zeros((size, self.state.shape[2]), f32)
            else:
                running = self.middle[1, rows, :].astype(f32)
            for n, d in enumerate(order):
                self.ready[d, rows, :] = running.astype(bf16)
                if leads or n < group - 1:
                    kept = carries[d, pl.ds(mine * per + q, 1), :]
                    running = kept * running + self.landed[d, rows, :].astype(f32)
            if leads:
                self.middle[0, rows, :] = running.astype(bf16)
        if leads:
            self.across().start()
        each(group, lambda t: self.second(t).start(), 1)
        self.entering[mine] = self.ready[mine]

    def finish(self):
        each(self.at.group, lambda t: self.second_in(t).wait_recv(), 1)

    def drain(self):
        each(self.at.group, lambda t: self.first(t).wait_send(), 1)
        each(self.at.group, lambda t: self.second(t).wait_send(), 1)

        @pl.when(self.at.part == self.leader)
        def _():
            self.across().wait_send()


def train_kernel(n_dp, n_seq, names, *refs):
    r = Refs(names, refs)
    at = Spot(n_dp, n_seq)
    inner, tokens = r.xt.shape
    heads = r.decay.shape[1]
    size = inner // heads
    ns = r.proj.shape[1] // 2
    share, model = r.rows.shape
    g = inner // LANES
    blocks = tokens // LANES
    head_rows = [slice(h * size, (h + 1) * size) for h in range(heads)]
    gather, scatter = Gather(at, r), Scatter(at, r)
    fore = Exchange(
        at, False, r.state, r.landed, r.ready, r.entering, r.middle,
        (r.s_send, r.s_recv, r.r_send, r.r_recv, r.m_send, r.m_recv),
    )
    rear = Exchange(
        at, True, r.b_state, r.b_landed, r.b_ready, r.leaving, r.b_middle,
        (r.bs_send, r.bs_recv, r.br_send, r.br_recv, r.bm_send, r.bm_recv),
    )
    b, c = slice(0, ns), slice(ns, 2 * ns)

    def wide(column):
        return jnp.concatenate([column] * blocks, axis=1)

    def lead(t):
        return remote(
            r.carries.at[at.spot], r.carries.at[at.spot],
            r.c_send.at[t], r.c_recv.at[t], at.group_peer(t),
        )

    def lead_in(t):
        p = (at.spot + at.group - t) % at.group
        return remote(
            r.carries.at[p], r.carries.at[p], r.c_send.at[t], r.c_recv.at[t], at.group_peer(t)
        )

    plane = n_dp * at.lows
    place = at.dp * at.lows + at.low

    def plane_edge(t, slot):
        return remote(
            r.gain_a.at[place], r.gain_a.at[slot],
            r.pa_send.at[t], r.pa_recv.at[t], at.plane_peer(t),
        )

    def line_edge(t, slot):
        return remote(
            r.gain_b.at[at.high], r.gain_b.at[slot],
            r.pb_send.at[t], r.pb_recv.at[t], at.high_peer(t),
        )

    def load(k, ref, to):
        return pltpu.make_async_copy(ref, to, r.l_sem.at[k])

    loads = [
        load(0, r.x_in, r.x), load(1, r.proj_in, r.proj),
        load(2, r.z_in, r.z), load(3, r.target_in, r.target),
    ]
    at.greet()
    for one in loads:
        one.start()
    r.held[...] = r.rows[...]
    for k, ref in enumerate((r.decay, r.bias, r.skip)):
        sub, lane = iota((heads, heads), 0), iota((heads, heads), 1)
        own = lane_total(jnp.where(sub == lane, ref[...], 0.0))
        row = to_row(own, k)
        packed = row if k == 0 else packed + row
    r.params[...] = packed
    r.gain_now[...] = r.gain[...]
    r.upper[...] = (iota((tokens, tokens), 0) <= iota((tokens, tokens), 1)).astype(bf16)
    loads[0].wait()
    for k in range(g):
        cols = slice(k * LANES, (k + 1) * LANES)
        r.xt[cols, :] = r.x[:, cols].astype(f32).T
    loads[1].wait()
    stop = jnp.where(r.ids[...] == 0, 1.0, 0.0)
    r.seg[...] = dot(jnp.broadcast_to(stop, (16, tokens)).astype(bf16), r.upper[...])

    def prepare():
        loads[2].wait()
        loads[3].wait()
        seg_c = r.seg[...].T[:, 0:1]
        raw = contract(r.proj[:, b], r.proj[:, c], 1, 1)
        open_to = (seg_c == r.seg[0:1, :]) & (
            iota((tokens, tokens), 0) <= iota((tokens, tokens), 1)
        )
        r.score[...] = jnp.where(open_to, raw, 0.0)
        for k in range(g):
            cols = slice(k * LANES, (k + 1) * LANES)
            zt = r.z[:, cols].astype(f32).T
            r.gate[cols, :] = zt * jax.nn.sigmoid(zt)

    def forward_head(h):
        rows = head_rows[h]
        for jb in range(blocks):
            js = slice(jb * LANES, (jb + 1) * LANES)
            left = r.sums_c[js, h : h + 1]
            for ib in range(jb, blocks):
                cs = slice(ib * LANES, (ib + 1) * LANES)
                gap = r.sums[h : h + 1, cs] - left
                if ib == jb:
                    gap = jnp.minimum(gap, 0.0)
                r.grid[h, js, cs] = (jnp.exp2(gap) * r.score[js, cs]).astype(bf16)
        for ib in range(blocks):
            end = (ib + 1) * LANES
            cs = slice(ib * LANES, end)
            r.mixed[rows, cs] = dot(r.scaled[rows, :end], r.grid[h, :end, cs])

    def backward_head(h):
        rows = head_rows[h]
        for jb in range(blocks):
            at_j = jb * LANES
            js = slice(at_j, at_j + LANES)
            part = contract(r.slope[rows, at_j:], r.grid[h, js, at_j:], 1, 1)
            r.col_dot[h : h + 1, js] = total(part * r.xt[rows, js])

    def own_state():
        packed = r.params[...]
        rate = -jnp.exp(jnp.broadcast_to(to_column(packed, 0, heads), (heads, tokens)))
        bias = jnp.broadcast_to(to_column(packed, 1, heads), (heads, tokens))
        w = jax.nn.softplus(r.raw_t[...] + bias)
        sums = accumulate(w * (rate * log2e), r.upper[...], 0)
        seg = r.seg[...][:heads]
        final = sums[:, tokens - 1 : tokens]
        last = seg[:, tokens - 1 : tokens]
        tail = jnp.where(seg == last, jnp.exp2(final - sums), 0.0)
        r.rate[...] = rate
        r.bias_w[...] = bias
        r.width[...] = w
        r.sums[...] = sums
        r.tail[...] = tail
        r.ending[...] = w * tail
        r.entry[...] = jnp.where(seg == 0.0, jnp.exp2(sums), 0.0)
        r.carries[at.spot] = jnp.broadcast_to(
            jnp.where(last == 0.0, jnp.exp2(final), 0.0), (heads, LANES)
        )
        for h in range(heads):
            rows = head_rows[h]
            r.slope[rows, :] = (r.xt[rows, :] * r.ending[h : h + 1, :]).astype(bf16)
        ended = dot(r.slope[...], r.proj[:, b])
        r.state[...] = ended.reshape(r.state.shape).astype(bf16)

    def open_step():
        each(at.group, lambda t: lead(t).start(), 1)
        fore.start()

    def step(s, _):
        r.sums_c[...] = r.sums[...].T
        for h in range(heads):
            rows = head_rows[h]
            r.scaled[rows, :] = (r.xt[rows, :] * r.width[h : h + 1, :]).astype(bf16)

        @pl.when(s == 0)
        def _():
            prepare()

        for k in range(g):
            row = jnp.broadcast_to(r.gain_now[k : k + 1, :], (LANES, LANES))
            r.gain_w[k * LANES : (k + 1) * LANES, :] = row.T
        cut = heads // 8
        marks = [slice(k * cut, (k + 1) * cut) for k in range(8)]

        def forward(k):
            for h in range(heads)[marks[k]]:
                forward_head(h)

        def backward(k):
            for h in range(heads)[marks[k]]:
                backward_head(h)

        forward(0)
        gather.from_low(0)
        forward(1)
        gather.from_high()
        each(at.group, lambda t: lead_in(t).wait_recv(), 1)
        fore.lead(r.carries, size)
        for u in range(1, at.highs):
            gather.from_low(u)
        for k in range(2, 5):
            forward(k)
        fore.follow(r.carries, size)
        for k in range(5, 8):
            forward(k)
        gather.from_y()
        fore.finish()

        passed = contract(flat(r.entering[...]), r.proj[:, c], 1, 1)
        skip = jnp.broadcast_to(to_column(r.params[...], 2, heads), (heads, tokens))
        r.skip_w[...] = skip
        power = jnp.zeros((8, tokens), f32)
        for h in range(heads):
            rows = head_rows[h]
            y = r.mixed[rows, :] + passed[rows, :] * r.entry[h : h + 1, :]
            r.mixed[rows, :] = y
            gated = (y + r.skip_w[h : h + 1, :] * r.xt[rows, :]) * r.gate[rows, :]
            r.gated[rows, :] = gated
            power = power + fold(gated * gated)
        root = lax.rsqrt(total(power) * (1.0 / inner) + norm_floor)
        r.root[...] = jnp.broadcast_to(root, r.root.shape)
        for k in range(g):
            rows = slice(k * LANES, (k + 1) * LANES)
            normed = r.gated[rows, :] * wide(r.gain_w[rows, :]) * r.root[0:1, :]
            r.normed[rows, :] = normed.astype(bf16)
            r.normed_n[:, rows] = normed.T.astype(bf16)

        gather.from_core()
        r.residual[...] = dot(r.normed_n[...], flat(r.full[...]))
        count = r.counts[0]
        for k in range(1, n_dp):
            count = count + r.counts[k]
        share_of = 1.0 / (model * count.astype(f32))
        limit = r.counts[at.dp] - at.seq * tokens
        lost = jnp.zeros((8, model), f32)
        step_rows = 32
        for q in range(tokens // step_rows):
            rows = slice(q * step_rows, (q + 1) * step_rows)
            scored = iota((step_rows, model), 0) + q * step_rows < limit
            gap = jnp.where(scored, r.residual[rows, :] - r.target[rows, :].astype(f32), 0.0)
            lost = lost + fold(gap * gap)
            r.og[rows, :] = (gap * (2.0 * share_of)).astype(bf16)
        loss = lane_total(total(lost)) * share_of

        def weight_part(t, y):
            dp = y * at.cores + (at.core + t) % at.cores
            width = n_seq * share
            left = r.normed[pl.ds(pl.multiple_of(dp * width, width), width), :]
            out = dot(left, r.og[...])
            r.grad[pl.ds(dp * n_seq, n_seq)] = out.reshape(n_seq, share, model).astype(bf16)
            if t > 0:
                scatter.core_edge(t, y).start()

        for t in range(1, at.cores):
            for u in range(at.ys):
                weight_part(t, (at.y + 1 + u) % at.ys)
        for u in range(at.ys):
            weight_part(0, (at.y + 1 + u) % at.ys)
        r.ng[...] = contract(flat(r.full[...]), r.og[...], 1, 1)
        scatter.to_y()
        inward = jnp.zeros((8, tokens), f32)
        for h in range(heads):
            rows = head_rows[h]
            lifted = r.ng[rows, :] * r.gated[rows, :]
            inward = inward + fold(lifted * wide(r.gain_w[rows, :]))
            lifted = lifted * r.root[0:1, :]
            part = lifted[:, :LANES]
            for k in range(1, blocks):
                part = part + lifted[:, k * LANES : (k + 1) * LANES]
            r.gain_part[rows, :] = part
        root = r.root[0:1, :]
        inward = total(inward) * (root * root * root * (1.0 / inner))
        r.inward[...] = jnp.broadcast_to(inward, r.inward.shape)
        for h in range(heads):
            rows = head_rows[h]
            dy = r.ng[rows, :] * wide(r.gain_w[rows, :]) * r.root[0:1, :]
            dy = (dy - r.gated[rows, :] * r.inward[0:1, :]) * r.gate[rows, :]
            r.row_dot[h : h + 1, :] = total(dy * r.mixed[rows, :])
            r.skip_dot[h : h + 1, :] = total(dy * r.xt[rows, :])
            r.slope[rows, :] = dy.astype(bf16)
            r.scaled[rows, :] = (dy * r.entry[h : h + 1, :]).astype(bf16)
        pulled = dot(r.scaled[...], r.proj[:, c])
        r.b_state[...] = pulled.reshape(r.b_state.shape).astype(bf16)
        rear.start()
        for k in range(g):
            rows = slice(k * LANES, (k + 1) * LANES)
            r.gain_a[place, k : k + 1, :] = total(r.gain_part[rows, :].T)
        each(plane, lambda t: plane_edge(t, place).start(), 1)
        backward(0)
        for u in range(at.highs):
            scatter.to_low(u)
            if u < 3:
                backward(u + 1)
            if u == 2:
                rear.lead(r.carries, size)
        backward(4)
        for t in range(1, at.highs):
            scatter.to_high(t)
        rear.follow(r.carries, size)
        for k in range(5, 8):
            backward(k)
        each(plane, lambda t: plane_edge(t, (place + plane - t) % plane).wait_recv(), 1)
        gain_sum = r.gain_a[0]
        for k in range(1, plane):
            gain_sum = gain_sum + r.gain_a[k]
        r.gain_b[at.high] = gain_sum
        each(at.highs, lambda t: line_edge(t, at.high).start(), 1)
        gather.drain()
        square = scatter.finish()
        rear.finish()

        after = flat(r.leaving[...])
        moved = contract(after, r.proj[:, b], 1, 1)
        for h in range(heads):
            rows = head_rows[h]
            r.pulled[h : h + 1, :] = total(moved[rows, :] * r.xt[rows, :])
        piece = r.leaving.shape[1]
        for h in range(heads):
            p, q = (h * size) // piece, (h * size) % piece
            own = r.leaving[p, q : q + size, :].astype(f32)
            own = own * r.entering[p, q : q + size, :].astype(f32)
            r.kept[h : h + 1, :] = total(own)
        drawn = r.pulled[...] * r.tail[...]
        w, rate = r.width[...], r.rate[...]
        col = r.col_dot[...] + drawn
        d_final = lane_total(w * drawn) + lane_total(r.kept[...] * r.carries[at.spot])
        d_rate = accumulate(r.row_dot[...] - w * col, r.upper[...], 1) + d_final
        d_width = (col + rate * d_rate) * jax.nn.sigmoid(r.raw_t[...] + r.bias_w[...])
        message = (
            to_row(lane_total(rate * d_rate * w), 0)
            + to_row(lane_total(d_width), 1)
            + to_row(lane_total(r.skip_dot[...]), 2)
        )
        lane = iota((1, LANES), 1)
        message = message + jnp.where(lane == 3 * heads, loss, 0.0)
        message = message + jnp.where(lane == 3 * heads + 1, square, 0.0)
        r.inbox[s, at.me] = message

        def news(t, slot):
            return remote(
                r.inbox.at[s, at.me], r.inbox.at[s, slot],
                r.n_send.at[t], r.n_recv.at[t], at.any_peer(t),
            )

        each(at.n, lambda t: news(t, at.me).start(), 1)
        each(at.highs, lambda t: line_edge(t, (at.high + at.highs - t) % at.highs).wait_recv(), 1)
        gain_sum = r.gain_b[0]
        for k in range(1, at.highs):
            gain_sum = gain_sum + r.gain_b[k]
        scatter.drain()
        fore.drain()
        rear.drain()
        each(at.group, lambda t: lead(t).wait_send(), 1)
        each(plane, lambda t: plane_edge(t, place).wait_send(), 1)
        each(at.highs, lambda t: line_edge(t, at.high).wait_send(), 1)
        each(at.n, lambda t: news(t, (at.me + at.n - t) % at.n).wait_recv(), 1)
        each(at.n, lambda t: news(t, at.me).wait_send(), 1)
        sums = jnp.sum(r.inbox[s], axis=0)
        small = jnp.where(lane < 3 * heads, sums, 0.0)
        norm = lane_total(small * small + total(gain_sum * gain_sum))
        norm = norm + lane_total(jnp.where(lane == 3 * heads + 1, sums, 0.0))
        pace = learn_rate * clip_limit / jnp.maximum(jnp.sqrt(norm), clip_limit)
        r.held[...] = r.held[...] - pace * r.acc[...]
        r.params[...] = r.params[...] - pace * small
        r.gain_now[...] = r.gain_now[...] - pace * gain_sum
        r.out_small[pl.ds(s + 1, 1), :] = jnp.broadcast_to(
            lane_total(jnp.where(lane == 3 * heads, sums, 0.0)), (1, LANES)
        )

        @pl.when(s < STEPS - 1)
        def _():
            r.full[at.me] = r.held[...].astype(bf16)
            gather.start()
            own_state()
            open_step()

        return 0

    r.full[at.me] = r.held[...].astype(bf16)
    own_state()
    at.meet()
    gather.start()
    open_step()
    lax.fori_loop(0, STEPS, step, 0)
    r.out_small[0:1, :] = r.params[...]
    r.out_gain[...] = r.gain_now[...]
    r.out_rows[...] = r.held[...]


def finish_kernel(rows, small, gain, losses, new_rows, decay, bias, skip, new_gain):
    heads = decay.shape[1]
    new_rows[...] = rows[...]
    new_gain[...] = gain[...]
    for k, ref in enumerate((decay, bias, skip)):
        ref[...] = small[0:1, k * heads : (k + 1) * heads]
    lane = iota((1, LANES), 1)
    both = jnp.where(lane == 0, small[1:2, :], small[2:3, :])
    losses[...] = both[:, :STEPS]


def call(body, outs, args, scratch=(), far=(), **extra):
    def place(k, a):
        if k in far:
            return pl.BlockSpec(memory_space=pl.ANY)
        return SMEM if a.ndim == 1 else VMEM

    return pl.pallas_call(
        body,
        out_shape=tuple(jax.ShapeDtypeStruct(*o) for o in outs),
        in_specs=[place(k, a) for k, a in enumerate(args)],
        out_specs=tuple([VMEM] * len(outs)),
        scratch_shapes=list(scratch),
        compiler_params=pltpu.CompilerParams(vmem_limit_bytes=LIMIT, **extra),
    )(*args)


def per_device(
    n_dp,
    n_seq,
    head_inputs,
    gate_inputs,
    state_proj,
    time_steps,
    token_ids,
    token_counts,
    teacher_out,
    out_weight,
    decay_log,
    step_bias,
    skip_gain,
    norm_gain,
):
    n = n_dp * n_seq
    x, z, target, raw = head_inputs[0], gate_inputs[0], teacher_out[0], time_steps[0]
    tokens, inner = x.shape
    ns = state_proj.shape[2] // 2
    heads = decay_log.shape[0]
    model = target.shape[1]
    share = out_weight.shape[0]
    group = n_seq // 2
    piece = inner // group
    g = inner // LANES
    cores = 2 if n_dp % 2 == 0 else 1
    ys = n_dp // cores
    highs = 4 if n_seq % 4 == 0 else n_seq
    lows = n_seq // highs
    per_head, tall = ((heads, tokens), f32), (inner, tokens)
    state = ((group, piece, ns), bf16)
    dma = pltpu.SemaphoreType.DMA
    vmem = {
        "x": (x.shape, bf16),
        "z": (z.shape, bf16),
        "target": (target.shape, bf16),
        "proj": (state_proj.shape[1:], bf16),
        "xt": (tall, f32),
        "gate": (tall, f32),
        "mixed": (tall, f32),
        "gated": (tall, f32),
        "ng": (tall, f32),
        "scaled": (tall, bf16),
        "slope": (tall, bf16),
        "normed": (tall, bf16),
        "normed_n": ((tokens, inner), bf16),
        "residual": ((tokens, model), f32),
        "og": ((tokens, model), bf16),
        "upper": ((tokens, tokens), bf16),
        "score": ((tokens, tokens), f32),
        "grid": ((heads, tokens, tokens), bf16),
        "seg": ((16, tokens), f32),
        "sums_c": ((tokens, heads), f32),
        "rate": per_head,
        "bias_w": per_head,
        "skip_w": per_head,
        "width": per_head,
        "sums": per_head,
        "tail": per_head,
        "ending": per_head,
        "entry": per_head,
        "row_dot": per_head,
        "skip_dot": per_head,
        "col_dot": per_head,
        "pulled": per_head,
        "kept": ((heads, ns), f32),
        "root": ((8, tokens), f32),
        "inward": ((8, tokens), f32),
        "gain_w": ((inner, LANES), f32),
        "gain_part": ((inner, LANES), f32),
        "gain_now": ((g, LANES), f32),
        "params": ((1, LANES), f32),
        "held": ((share, model), f32),
        "acc": ((share, model), f32),
        "full": ((n, share, model), bf16),
        "grad": ((n, share, model), bf16),
        "from_core": ((cores * ys, n_seq, share, model), bf16),
        "staged1": ((n // cores, share, model), bf16),
        "from1": ((n // cores, share, model), bf16),
        "staged2": ((n_seq, share, model), bf16),
        "from2": ((n_seq, share, model), bf16),
        "staged3": ((highs, share, model), bf16),
        "from3": ((highs, share, model), bf16),
        "middle": ((2, piece, ns), bf16),
        "b_middle": ((2, piece, ns), bf16),
        "state": state,
        "landed": state,
        "ready": state,
        "entering": state,
        "b_state": state,
        "b_landed": state,
        "b_ready": state,
        "leaving": state,
        "carries": ((group, heads, LANES), f32),
        "gain_a": ((n_dp * lows, g, LANES), f32),
        "gain_b": ((highs, g, LANES), f32),
        "inbox": ((STEPS, n, 1, LANES), f32),
    }
    sems = {
        "l_sem": (4,),
        "w_recv": (n,),
        "wz_send": (highs,),
        "wx_send": (n_seq,),
        "wy_send": (n // cores,),
        "wc_send": (n,),
        "gc_send": (cores * ys,),
        "gc_recv": (cores * ys,),
        "g1_send": (n // cores,),
        "g1_recv": (n // cores,),
        "g2_send": (n_seq,),
        "g2_recv": (n_seq,),
        "g3_send": (highs,),
        "g3_recv": (highs,),
        "m_send": (1,),
        "m_recv": (1,),
        "bm_send": (1,),
        "bm_recv": (1,),
        "pa_send": (n_dp * lows,),
        "pa_recv": (n_dp * lows,),
        "pb_send": (highs,),
        "pb_recv": (highs,),
        "n_send": (n,),
        "n_recv": (n,),
    }
    for name in ("c", "s", "r", "bs", "br"):
        sems[name + "_send"] = (group,)
        sems[name + "_recv"] = (group,)
    given = {
        "counts": token_counts,
        "decay": decay_log.reshape(1, heads),
        "bias": step_bias.reshape(1, heads),
        "skip": skip_gain.reshape(1, heads),
        "gain": norm_gain.reshape(g, LANES),
        "raw_t": raw.T,
        "ids": token_ids,
        "x_in": x,
        "z_in": z,
        "target_in": target,
        "proj_in": state_proj[0],
        "rows": out_weight,
    }
    outs = {
        "out_rows": ((share, model), f32),
        "out_small": ((8, LANES), f32),
        "out_gain": ((g, LANES), f32),
    }
    far = [k for k, name in enumerate(given) if name.endswith("_in")]
    names = [*given, *outs, *vmem, *sems]
    rows, small, gain = call(
        functools.partial(train_kernel, n_dp, n_seq, names),
        outs.values(),
        tuple(given.values()),
        [pltpu.VMEM(*v) for v in vmem.values()] + [dma(v) for v in sems.values()],
        far,
        collective_id=0,
        has_side_effects=True,
    )
    losses, rows, decay, bias, skip, gain = call(
        finish_kernel,
        [
            ((1, STEPS), f32),
            ((share, model), f32),
            ((1, heads), f32),
            ((1, heads), f32),
            ((1, heads), f32),
            ((g, LANES), f32),
        ],
        (rows, small, gain),
    )
    return (
        losses.reshape(STEPS),
        rows,
        decay.reshape(heads),
        bias.reshape(heads),
        skip.reshape(heads),
        gain.reshape(inner),
    )


def solution(mesh):
    in_specs = (
        P("dp", "seq", None),
        P("dp", "seq", None),
        P("dp", "seq", None),
        P("dp", "seq", None),
        P("dp", "seq"),
        P(),
        P("dp", "seq", None),
        P(("dp", "seq"), None),
        P(),
        P(),
        P(),
        P(),
    )
    out_specs = (P(), P(("dp", "seq"), None), P(), P(), P(), P())
    return jax.shard_map(
        functools.partial(per_device, mesh.shape["dp"], mesh.shape["seq"]),
        mesh=mesh,
        in_specs=in_specs,
        out_specs=out_specs,
        check_vma=False,
    )
```

```python
import functools

import jax
import jax.numpy as jnp
from jax import lax
from jax.experimental import pallas as pl
from jax.experimental.pallas import tpu as pltpu
from jax.sharding import PartitionSpec as P

STEPS = 2
norm_floor = 1.0
clip_limit = 1.0
learn_rate = 8.0
log2e = 1.4426950408889634
f32 = jnp.float32
bf16 = jnp.bfloat16
LANES = 128
VMEM = pl.BlockSpec(memory_space=pltpu.VMEM)
SMEM = pl.BlockSpec(memory_space=pltpu.SMEM)
MESH = pl.DeviceIdType.MESH
LIMIT = 60 * 1024 * 1024


def dot(a, b):
    return jnp.dot(a, b, preferred_element_type=f32)


def contract(a, b, da, db):
    return lax.dot_general(a, b, (((da,), (db,)), ((), ())), preferred_element_type=f32)


def iota(shape, axis):
    return lax.broadcasted_iota(jnp.int32, shape, axis)


def fold(a):
    rows, width = a.shape
    return jnp.sum(a.reshape(rows // 8, 8, width), axis=0)


def total(a):
    return jnp.sum(a, axis=0, keepdims=True)


def lane_total(a):
    return jnp.sum(a, axis=1, keepdims=True)


def flat(a):
    k, rows, width = a.shape
    if rows % 16 == 0 or a.dtype == f32:
        return a.reshape(k * rows, width)
    return a.astype(f32).reshape(k * rows, width).astype(a.dtype)


def each(n, body, first=0):
    if n - first <= 3:
        for t in range(first, n):
            body(t)
        return

    def one(t, _):
        body(t)
        return 0

    lax.fori_loop(first, n, one, 0)


def remote(source, target, send, recv, peer):
    return pltpu.make_async_remote_copy(
        src_ref=source,
        dst_ref=target,
        send_sem=send,
        recv_sem=recv,
        device_id=peer,
        device_id_type=MESH,
    )


class Refs:
    def __init__(self, names, refs):
        self.__dict__.update(zip(names, refs))


class Spot:
    def __init__(self, n_dp, n_seq):
        self.n_dp, self.n_seq, self.n = n_dp, n_seq, n_dp * n_seq
        self.cores = 2 if n_dp % 2 == 0 else 1
        self.ys = n_dp // self.cores
        self.highs = 4 if n_seq % 4 == 0 else n_seq
        self.lows = n_seq // self.highs
        self.dp, self.seq = lax.axis_index("dp"), lax.axis_index("seq")
        self.y, self.core = self.dp // self.cores, self.dp % self.cores
        self.high, self.low = self.seq // self.lows, self.seq % self.lows
        self.me = self.dp * n_seq + self.seq
        self.group = n_seq // 2
        self.part, self.spot = self.seq // self.group, self.seq % self.group

    def core_peer(self, t):
        return (self.y * self.cores + (self.core + t) % self.cores, self.seq)

    def y_peer(self, t):
        return (((self.y + t) % self.ys) * self.cores + self.core, self.seq)

    def low_peer(self, t):
        return (self.dp, self.high * self.lows + (self.low + t) % self.lows)

    def high_peer(self, t):
        return (self.dp, ((self.high + t) % self.highs) * self.lows + self.low)

    def group_peer(self, t):
        return (self.dp, self.part * self.group + (self.spot + t) % self.group)

    def other_half(self):
        return (self.dp, (self.seq + self.group) % self.n_seq)

    def any_peer(self, t):
        to = (self.me + t) % self.n
        return (to // self.n_seq, to % self.n_seq)

    def plane_peer(self, t):
        to = (self.dp * self.lows + self.low + t) % (self.n_dp * self.lows)
        return (to // self.lows, self.high * self.lows + to % self.lows)

    def chunk(self, y, high, low):
        return (y * self.cores + self.core) * self.n_seq + high * self.lows + low

    def near(self):
        return [
            (self.highs, self.high_peer),
            (self.group, self.group_peer),
            (2, lambda t: self.other_half()),
            (self.n_dp * self.lows, self.plane_peer),
        ]

    def greet(self):
        barrier = pltpu.get_barrier_semaphore()
        for count, peer in self.near():
            each(
                count,
                lambda t, peer=peer: pl.semaphore_signal(
                    barrier, inc=1, device_id=peer(t), device_id_type=MESH
                ),
                1,
            )

    def meet(self):
        count = sum(count - 1 for count, _ in self.near())
        pl.semaphore_wait(pltpu.get_barrier_semaphore(), count)


def to_column(row, k, heads):
    sub, lane = iota((heads, LANES), 0), iota((heads, LANES), 1)
    return lane_total(jnp.where(lane == k * heads + sub, row, 0.0))


def to_row(column, k):
    heads = column.shape[0]
    sub, lane = iota((heads, LANES), 0), iota((heads, LANES), 1)
    return total(jnp.where(lane == k * heads + sub, column, 0.0))


def accumulate(a, upper, axis):
    rows = a.shape[0]
    high = a.astype(bf16)
    rest = a - high.astype(f32)
    mid = rest.astype(bf16)
    low = (rest - mid.astype(f32)).astype(bf16)
    out = contract(jnp.concatenate([high, mid, low], axis=0), upper, 1, axis)
    return out[:rows] + out[rows : 2 * rows] + out[2 * rows :]


class Gather:
    def __init__(self, at, r):
        self.at, self.r = at, r

    def push(self, chunk, send, peer):
        r = self.r
        return remote(r.full.at[chunk], r.full.at[chunk], send, r.w_recv.at[chunk], peer)

    def arrived(self, chunk):
        self.push(chunk, self.r.wz_send.at[0], self.at.core_peer(1)).wait_recv()

    def high_edge(self, t):
        return self.push(self.at.me, self.r.wz_send.at[t], self.at.high_peer(t))

    def low_edge(self, t, high):
        at = self.at
        chunk = at.chunk(at.y, high, at.low)
        return self.push(chunk, self.r.wx_send.at[t * at.highs + high], at.low_peer(t))

    def y_edge(self, t, high, low):
        at = self.at
        send = self.r.wy_send.at[(t * at.highs + high) * at.lows + low]
        return self.push(at.chunk(at.y, high, low), send, at.y_peer(t))

    def core_edge(self, t, y, seq):
        at = self.at
        send = self.r.wc_send.at[(t * at.ys + y) * at.n_seq + seq]
        return self.push((y * at.cores + at.core) * at.n_seq + seq, send, at.core_peer(t))

    def onward(self, y, high, low, to_low, to_y):
        at = self.at
        if to_low:
            each(at.lows, lambda t: self.low_edge(t, high).start(), 1)
        if to_y:
            each(at.ys, lambda t: self.y_edge(t, high, low).start(), 1)
        each(at.cores, lambda t: self.core_edge(t, y, high * at.lows + low).start(), 1)

    def start(self):
        at = self.at
        each(at.highs, lambda t: self.high_edge(t).start(), 1)
        self.onward(at.y, at.high, at.low, True, True)

    def from_high(self):
        at = self.at

        def one(t):
            high = (at.high + at.highs - t) % at.highs
            self.arrived(at.chunk(at.y, high, at.low))
            self.onward(at.y, high, at.low, True, True)

        each(at.highs, one, 1)

    def from_low(self, u):
        at = self.at
        high = (at.high + at.highs - u) % at.highs

        def pick(t):
            low = (at.low + at.lows - t) % at.lows
            self.arrived(at.chunk(at.y, high, low))
            self.onward(at.y, high, low, False, True)

        each(at.lows, pick, 1)

    def from_y(self):
        at = self.at

        def one(t, v):
            y = (at.y + at.ys - t) % at.ys
            high = (at.high + at.highs - v % at.highs) % at.highs
            low = (at.low + v // at.highs) % at.lows
            self.arrived(at.chunk(y, high, low))
            self.onward(y, high, low, False, False)

        each(at.ys, lambda t: each(at.n_seq, lambda v: one(t, v)), 1)

    def from_core(self):
        at = self.at

        def one(t, v):
            core = (at.core + t) % at.cores
            self.arrived(((v // at.n_seq) * at.cores + core) * at.n_seq + v % at.n_seq)

        each(at.cores, lambda t: each(at.ys * at.n_seq, lambda v: one(t, v)), 1)

    def drain(self):
        at = self.at
        each(at.highs, lambda t: self.high_edge(t).wait_send(), 1)
        each(at.lows, lambda t: each(at.highs, lambda u: self.low_edge(t, u).wait_send()), 1)
        each(
            at.ys,
            lambda t: each(
                at.n_seq, lambda v: self.y_edge(t, v // at.lows, v % at.lows).wait_send()
            ),
            1,
        )
        each(
            at.cores,
            lambda t: each(
                at.ys * at.n_seq,
                lambda v: self.core_edge(t, v // at.n_seq, v % at.n_seq).wait_send(),
            ),
            1,
        )


class Scatter:
    def __init__(self, at, r):
        self.at, self.r = at, r

    def core_edge(self, t, y):
        at, r = self.at, self.r
        dp = y * at.cores + (at.core + t) % at.cores
        slot = t * at.ys + y
        return remote(
            r.grad.at[pl.ds(dp * at.n_seq, at.n_seq)], r.from_core.at[slot],
            r.gc_send.at[slot], r.gc_recv.at[slot], at.core_peer(t),
        )

    def y_edge(self, t, high, low):
        at, r = self.at, self.r
        slot = (t * at.highs + high) * at.lows + low
        return remote(
            r.staged1.at[slot], r.from1.at[slot],
            r.g1_send.at[slot], r.g1_recv.at[slot], at.y_peer(t),
        )

    def low_edge(self, t, high):
        at, r = self.at, self.r
        slot = t * at.highs + high
        return remote(
            r.staged2.at[slot], r.from2.at[slot],
            r.g2_send.at[slot], r.g2_recv.at[slot], at.low_peer(t),
        )

    def high_edge(self, t):
        at, r = self.at, self.r
        return remote(
            r.staged3.at[t], r.from3.at[t], r.g3_send.at[t], r.g3_recv.at[t], at.high_peer(t)
        )

    def chip_sum(self, y, high, low):
        at, r = self.at, self.r
        acc = r.grad[at.chunk(y, high, low)].astype(f32)
        for t in range(1, at.cores):
            acc = acc + r.from_core[t * at.ys + y, high * at.lows + low].astype(f32)
        return acc

    def y_sum(self, high, low):
        at, r = self.at, self.r
        acc = self.chip_sum(at.y, high, low)
        for t in range(1, at.ys):
            self.y_edge(t, high, low).wait_recv()
            acc = acc + r.from1[(t * at.highs + high) * at.lows + low].astype(f32)
        return acc

    def low_sum(self, high):
        at, r = self.at, self.r
        acc = self.y_sum(high, at.low)
        for t in range(1, at.lows):
            self.low_edge(t, high).wait_recv()
            acc = acc + r.from2[t * at.highs + high].astype(f32)
        return acc

    def from_core(self, u):
        at = self.at
        each(at.cores, lambda t: self.core_edge(t, (at.y + u) % at.ys).wait_recv(), 1)

    def to_y(self):
        at, r = self.at, self.r
        each(at.ys, self.from_core, 1)

        def one(t, v):
            low = (at.low + 1 + v // at.highs) % at.lows
            high = (at.high + 1 + v) % at.highs
            acc = self.chip_sum((at.y + t) % at.ys, high, low)
            r.staged1[(t * at.highs + high) * at.lows + low] = acc.astype(bf16)
            self.y_edge(t, high, low).start()

        each(at.ys, lambda t: each(at.n_seq, lambda v: one(t, v)), 1)

    def to_low(self, u):
        at, r = self.at, self.r
        high = (at.high + 1 + u) % at.highs

        def one(t):
            low = (at.low + t) % at.lows
            r.staged2[t * at.highs + high] = self.y_sum(high, low).astype(bf16)
            self.low_edge(t, high).start()

        each(at.lows, one, 1)

    def to_high(self, t):
        at, r = self.at, self.r
        r.staged3[t] = self.low_sum((at.high + t) % at.highs).astype(bf16)
        self.high_edge(t).start()

    def finish(self):
        at, r = self.at, self.r
        acc = self.low_sum(at.high)
        each(at.highs, lambda t: self.high_edge(t).wait_recv(), 1)
        for t in range(1, at.highs):
            acc = acc + r.from3[t].astype(f32)
        r.acc[...] = acc
        return lane_total(total(fold(acc * acc)))

    def drain(self):
        at = self.at
        for t in range(1, at.cores):
            each(at.ys, lambda y: self.core_edge(t, y).wait_send())
        each(
            at.ys,
            lambda t: each(
                at.n_seq, lambda v: self.y_edge(t, v // at.lows, v % at.lows).wait_send()
            ),
            1,
        )
        each(at.lows, lambda t: each(at.highs, lambda u: self.low_edge(t, u).wait_send()), 1)
        each(at.highs, lambda t: self.high_edge(t).wait_send(), 1)


class Exchange:
    def __init__(self, at, reverse, state, landed, ready, entering, middle, sems):
        self.at, self.reverse = at, reverse
        self.state, self.landed, self.ready, self.entering = state, landed, ready, entering
        self.middle = middle
        self.s_send, self.s_recv, self.r_send, self.r_recv, self.m_send, self.m_recv = sems
        self.leader = 1 if reverse else 0

    def back(self, t):
        return (self.at.spot + self.at.group - t) % self.at.group

    def first(self, t):
        p = (self.at.spot + t) % self.at.group
        return remote(
            self.state.at[p], self.landed.at[self.at.spot],
            self.s_send.at[t], self.s_recv.at[t], self.at.group_peer(t),
        )

    def first_in(self, t):
        p = self.back(t)
        return remote(
            self.state.at[p], self.landed.at[p],
            self.s_send.at[t], self.s_recv.at[t], self.at.group_peer(t),
        )

    def second(self, t):
        p = (self.at.spot + t) % self.at.group
        return remote(
            self.ready.at[p], self.entering.at[self.at.spot],
            self.r_send.at[t], self.r_recv.at[t], self.at.group_peer(t),
        )

    def second_in(self, t):
        p = self.back(t)
        return remote(
            self.ready.at[p], self.entering.at[p],
            self.r_send.at[t], self.r_recv.at[t], self.at.group_peer(t),
        )

    def across(self):
        return remote(
            self.middle.at[0], self.middle.at[1],
            self.m_send.at[0], self.m_recv.at[0], self.at.other_half(),
        )

    def start(self):
        at = self.at
        each(at.group, lambda t: self.first(t).start(), 1)
        self.landed[at.spot] = self.state[at.spot]

    def lead(self, carries, size):
        @pl.when(self.at.part == self.leader)
        def _():
            self.turn(carries, size, True)

    def follow(self, carries, size):
        @pl.when(self.at.part != self.leader)
        def _():
            self.turn(carries, size, False)

    def turn(self, carries, size, leads):
        at = self.at
        mine, group = at.spot, at.group
        each(group, lambda t: self.first_in(t).wait_recv(), 1)
        if not leads:
            self.across().wait_recv()
        piece = self.state.shape[1]
        per = piece // size
        order = list(range(group))
        if self.reverse:
            order.reverse()
        for q in range(per):
            rows = slice(q * size, (q + 1) * size)
            if leads:
                running = jnp.zeros((size, self.state.shape[2]), f32)
            else:
                running = self.middle[1, rows, :].astype(f32)
            for n, d in enumerate(order):
                self.ready[d, rows, :] = running.astype(bf16)
                if leads or n < group - 1:
                    kept = carries[d, pl.ds(mine * per + q, 1), :]
                    running = kept * running + self.landed[d, rows, :].astype(f32)
            if leads:
                self.middle[0, rows, :] = running.astype(bf16)
        if leads:
            self.across().start()
        each(group, lambda t: self.second(t).start(), 1)
        self.entering[mine] = self.ready[mine]

    def finish(self):
        each(self.at.group, lambda t: self.second_in(t).wait_recv(), 1)

    def drain(self):
        each(self.at.group, lambda t: self.first(t).wait_send(), 1)
        each(self.at.group, lambda t: self.second(t).wait_send(), 1)

        @pl.when(self.at.part == self.leader)
        def _():
            self.across().wait_send()


def train_kernel(n_dp, n_seq, names, *refs):
    r = Refs(names, refs)
    at = Spot(n_dp, n_seq)
    inner, tokens = r.xt.shape
    heads = r.decay.shape[1]
    size = inner // heads
    ns = r.proj.shape[1] // 2
    share, model = r.rows.shape
    g = inner // LANES
    blocks = tokens // LANES
    head_rows = [slice(h * size, (h + 1) * size) for h in range(heads)]
    gather, scatter = Gather(at, r), Scatter(at, r)
    fore = Exchange(
        at, False, r.state, r.landed, r.ready, r.entering, r.middle,
        (r.s_send, r.s_recv, r.r_send, r.r_recv, r.m_send, r.m_recv),
    )
    rear = Exchange(
        at, True, r.b_state, r.b_landed, r.b_ready, r.leaving, r.b_middle,
        (r.bs_send, r.bs_recv, r.br_send, r.br_recv, r.bm_send, r.bm_recv),
    )
    b, c = slice(0, ns), slice(ns, 2 * ns)

    def wide(column):
        return jnp.concatenate([column] * blocks, axis=1)

    def lead(t):
        return remote(
            r.carries.at[at.spot], r.carries.at[at.spot],
            r.c_send.at[t], r.c_recv.at[t], at.group_peer(t),
        )

    def lead_in(t):
        p = (at.spot + at.group - t) % at.group
        return remote(
            r.carries.at[p], r.carries.at[p], r.c_send.at[t], r.c_recv.at[t], at.group_peer(t)
        )

    plane = n_dp * at.lows
    place = at.dp * at.lows + at.low

    def plane_edge(t, slot):
        return remote(
            r.gain_a.at[place], r.gain_a.at[slot],
            r.pa_send.at[t], r.pa_recv.at[t], at.plane_peer(t),
        )

    def line_edge(t, slot):
        return remote(
            r.gain_b.at[at.high], r.gain_b.at[slot],
            r.pb_send.at[t], r.pb_recv.at[t], at.high_peer(t),
        )

    def load(k, ref, to):
        return pltpu.make_async_copy(ref, to, r.l_sem.at[k])

    loads = [
        load(0, r.x_in, r.x), load(1, r.proj_in, r.proj),
        load(2, r.z_in, r.z), load(3, r.target_in, r.target),
    ]
    at.greet()
    for one in loads:
        one.start()
    r.held[...] = r.rows[...]
    for k, ref in enumerate((r.decay, r.bias, r.skip)):
        sub, lane = iota((heads, heads), 0), iota((heads, heads), 1)
        own = lane_total(jnp.where(sub == lane, ref[...], 0.0))
        row = to_row(own, k)
        packed = row if k == 0 else packed + row
    r.params[...] = packed
    r.gain_now[...] = r.gain[...]
    r.upper[...] = (iota((tokens, tokens), 0) <= iota((tokens, tokens), 1)).astype(bf16)
    loads[0].wait()
    for k in range(g):
        cols = slice(k * LANES, (k + 1) * LANES)
        r.xt[cols, :] = r.x[:, cols].astype(f32).T
    loads[1].wait()
    stop = jnp.where(r.ids[...] == 0, 1.0, 0.0)
    r.seg[...] = dot(jnp.broadcast_to(stop, (16, tokens)).astype(bf16), r.upper[...])

    def prepare():
        loads[2].wait()
        loads[3].wait()
        seg_c = r.seg[...].T[:, 0:1]
        raw = contract(r.proj[:, b], r.proj[:, c], 1, 1)
        open_to = (seg_c == r.seg[0:1, :]) & (
            iota((tokens, tokens), 0) <= iota((tokens, tokens), 1)
        )
        r.score[...] = jnp.where(open_to, raw, 0.0)
        for k in range(g):
            cols = slice(k * LANES, (k + 1) * LANES)
            zt = r.z[:, cols].astype(f32).T
            r.gate[cols, :] = zt * jax.nn.sigmoid(zt)

    def forward_head(h):
        rows = head_rows[h]
        for jb in range(blocks):
            js = slice(jb * LANES, (jb + 1) * LANES)
            left = r.sums_c[js, h : h + 1]
            for ib in range(jb, blocks):
                cs = slice(ib * LANES, (ib + 1) * LANES)
                gap = r.sums[h : h + 1, cs] - left
                if ib == jb:
                    gap = jnp.minimum(gap, 0.0)
                r.grid[h, js, cs] = (jnp.exp2(gap) * r.score[js, cs]).astype(bf16)
        for ib in range(blocks):
            end = (ib + 1) * LANES
            cs = slice(ib * LANES, end)
            r.mixed[rows, cs] = dot(r.scaled[rows, :end], r.grid[h, :end, cs])

    def backward_head(h):
        rows = head_rows[h]
        for jb in range(blocks):
            at_j = jb * LANES
            js = slice(at_j, at_j + LANES)
            part = contract(r.slope[rows, at_j:], r.grid[h, js, at_j:], 1, 1)
            r.col_dot[h : h + 1, js] = total(part * r.xt[rows, js])

    def own_state():
        packed = r.params[...]
        rate = -jnp.exp(jnp.broadcast_to(to_column(packed, 0, heads), (heads, tokens)))
        bias = jnp.broadcast_to(to_column(packed, 1, heads), (heads, tokens))
        w = jax.nn.softplus(r.raw_t[...] + bias)
        sums = accumulate(w * (rate * log2e), r.upper[...], 0)
        seg = r.seg[...][:heads]
        final = sums[:, tokens - 1 : tokens]
        last = seg[:, tokens - 1 : tokens]
        tail = jnp.where(seg == last, jnp.exp2(final - sums), 0.0)
        r.rate[...] = rate
        r.bias_w[...] = bias
        r.width[...] = w
        r.sums[...] = sums
        r.tail[...] = tail
        r.ending[...] = w * tail
        r.entry[...] = jnp.where(seg == 0.0, jnp.exp2(sums), 0.0)
        r.carries[at.spot] = jnp.broadcast_to(
            jnp.where(last == 0.0, jnp.exp2(final), 0.0), (heads, LANES)
        )
        for h in range(heads):
            rows = head_rows[h]
            r.slope[rows, :] = (r.xt[rows, :] * r.ending[h : h + 1, :]).astype(bf16)
        ended = dot(r.slope[...], r.proj[:, b])
        r.state[...] = ended.reshape(r.state.shape).astype(bf16)

    def open_step():
        each(at.group, lambda t: lead(t).start(), 1)
        fore.start()

    def step(s, _):
        r.sums_c[...] = r.sums[...].T
        for h in range(heads):
            rows = head_rows[h]
            r.scaled[rows, :] = (r.xt[rows, :] * r.width[h : h + 1, :]).astype(bf16)

        @pl.when(s == 0)
        def _():
            prepare()

        for k in range(g):
            row = jnp.broadcast_to(r.gain_now[k : k + 1, :], (LANES, LANES))
            r.gain_w[k * LANES : (k + 1) * LANES, :] = row.T
        cut = heads // 8
        marks = [slice(k * cut, (k + 1) * cut) for k in range(8)]

        def forward(k):
            for h in range(heads)[marks[k]]:
                forward_head(h)

        def backward(k):
            for h in range(heads)[marks[k]]:
                backward_head(h)

        forward(0)
        gather.from_low(0)
        forward(1)
        gather.from_high()
        each(at.group, lambda t: lead_in(t).wait_recv(), 1)
        fore.lead(r.carries, size)
        for u in range(1, at.highs):
            gather.from_low(u)
        for k in range(2, 5):
            forward(k)
        fore.follow(r.carries, size)
        for k in range(5, 8):
            forward(k)
        gather.from_y()
        fore.finish()

        passed = contract(flat(r.entering[...]), r.proj[:, c], 1, 1)
        skip = jnp.broadcast_to(to_column(r.params[...], 2, heads), (heads, tokens))
        r.skip_w[...] = skip
        power = jnp.zeros((8, tokens), f32)
        for h in range(heads):
            rows = head_rows[h]
            y = r.mixed[rows, :] + passed[rows, :] * r.entry[h : h + 1, :]
            r.mixed[rows, :] = y
            gated = (y + r.skip_w[h : h + 1, :] * r.xt[rows, :]) * r.gate[rows, :]
            r.gated[rows, :] = gated
            power = power + fold(gated * gated)
        root = lax.rsqrt(total(power) * (1.0 / inner) + norm_floor)
        r.root[...] = jnp.broadcast_to(root, r.root.shape)
        for k in range(g):
            rows = slice(k * LANES, (k + 1) * LANES)
            normed = r.gated[rows, :] * wide(r.gain_w[rows, :]) * r.root[0:1, :]
            r.normed[rows, :] = normed.astype(bf16)
            r.normed_n[:, rows] = normed.T.astype(bf16)

        gather.from_core()
        r.residual[...] = dot(r.normed_n[...], flat(r.full[...]))
        count = r.counts[0]
        for k in range(1, n_dp):
            count = count + r.counts[k]
        share_of = 1.0 / (model * count.astype(f32))
        limit = r.counts[at.dp] - at.seq * tokens
        lost = jnp.zeros((8, model), f32)
        step_rows = 32
        for q in range(tokens // step_rows):
            rows = slice(q * step_rows, (q + 1) * step_rows)
            scored = iota((step_rows, model), 0) + q * step_rows < limit
            gap = jnp.where(scored, r.residual[rows, :] - r.target[rows, :].astype(f32), 0.0)
            lost = lost + fold(gap * gap)
            r.og[rows, :] = (gap * (2.0 * share_of)).astype(bf16)
        loss = lane_total(total(lost)) * share_of

        def weight_part(t, y):
            dp = y * at.cores + (at.core + t) % at.cores
            width = n_seq * share
            left = r.normed[pl.ds(pl.multiple_of(dp * width, width), width), :]
            out = dot(left, r.og[...])
            r.grad[pl.ds(dp * n_seq, n_seq)] = out.reshape(n_seq, share, model).astype(bf16)
            if t > 0:
                scatter.core_edge(t, y).start()

        for t in range(1, at.cores):
            for u in range(at.ys):
                weight_part(t, (at.y + 1 + u) % at.ys)
        for u in range(at.ys):
            weight_part(0, (at.y + 1 + u) % at.ys)
        r.ng[...] = contract(flat(r.full[...]), r.og[...], 1, 1)
        scatter.to_y()
        inward = jnp.zeros((8, tokens), f32)
        for h in range(heads):
            rows = head_rows[h]
            lifted = r.ng[rows, :] * r.gated[rows, :]
            inward = inward + fold(lifted * wide(r.gain_w[rows, :]))
            lifted = lifted * r.root[0:1, :]
            part = lifted[:, :LANES]
            for k in range(1, blocks):
                part = part + lifted[:, k * LANES : (k + 1) * LANES]
            r.gain_part[rows, :] = part
        root = r.root[0:1, :]
        inward = total(inward) * (root * root * root * (1.0 / inner))
        r.inward[...] = jnp.broadcast_to(inward, r.inward.shape)
        for h in range(heads):
            rows = head_rows[h]
            dy = r.ng[rows, :] * wide(r.gain_w[rows, :]) * r.root[0:1, :]
            dy = (dy - r.gated[rows, :] * r.inward[0:1, :]) * r.gate[rows, :]
            r.row_dot[h : h + 1, :] = total(dy * r.mixed[rows, :])
            r.skip_dot[h : h + 1, :] = total(dy * r.xt[rows, :])
            r.slope[rows, :] = dy.astype(bf16)
            r.scaled[rows, :] = (dy * r.entry[h : h + 1, :]).astype(bf16)
        pulled = dot(r.scaled[...], r.proj[:, c])
        r.b_state[...] = pulled.reshape(r.b_state.shape).astype(bf16)
        rear.start()
        for k in range(g):
            rows = slice(k * LANES, (k + 1) * LANES)
            r.gain_a[place, k : k + 1, :] = total(r.gain_part[rows, :].T)
        each(plane, lambda t: plane_edge(t, place).start(), 1)
        backward(0)
        scatter.from_core(0)
        for u in range(at.highs):
            scatter.to_low(u)
            if u < 3:
                backward(u + 1)
            if u == 2:
                rear.lead(r.carries, size)
        backward(4)
        for t in range(1, at.highs):
            scatter.to_high(t)
        rear.follow(r.carries, size)
        for k in range(5, 8):
            backward(k)
        each(plane, lambda t: plane_edge(t, (place + plane - t) % plane).wait_recv(), 1)
        gain_sum = r.gain_a[0]
        for k in range(1, plane):
            gain_sum = gain_sum + r.gain_a[k]
        r.gain_b[at.high] = gain_sum
        each(at.highs, lambda t: line_edge(t, at.high).start(), 1)
        gather.drain()
        square = scatter.finish()
        rear.finish()

        after = flat(r.leaving[...])
        moved = contract(after, r.proj[:, b], 1, 1)
        for h in range(heads):
            rows = head_rows[h]
            r.pulled[h : h + 1, :] = total(moved[rows, :] * r.xt[rows, :])
        piece = r.leaving.shape[1]
        for h in range(heads):
            p, q = (h * size) // piece, (h * size) % piece
            own = r.leaving[p, q : q + size, :].astype(f32)
            own = own * r.entering[p, q : q + size, :].astype(f32)
            r.kept[h : h + 1, :] = total(own)
        drawn = r.pulled[...] * r.tail[...]
        w, rate = r.width[...], r.rate[...]
        col = r.col_dot[...] + drawn
        d_final = lane_total(w * drawn) + lane_total(r.kept[...] * r.carries[at.spot])
        d_rate = accumulate(r.row_dot[...] - w * col, r.upper[...], 1) + d_final
        d_width = (col + rate * d_rate) * jax.nn.sigmoid(r.raw_t[...] + r.bias_w[...])
        message = (
            to_row(lane_total(rate * d_rate * w), 0)
            + to_row(lane_total(d_width), 1)
            + to_row(lane_total(r.skip_dot[...]), 2)
        )
        lane = iota((1, LANES), 1)
        message = message + jnp.where(lane == 3 * heads, loss, 0.0)
        message = message + jnp.where(lane == 3 * heads + 1, square, 0.0)
        r.inbox[s, at.me] = message

        def news(t, slot):
            return remote(
                r.inbox.at[s, at.me], r.inbox.at[s, slot],
                r.n_send.at[t], r.n_recv.at[t], at.any_peer(t),
            )

        each(at.n, lambda t: news(t, at.me).start(), 1)
        each(at.highs, lambda t: line_edge(t, (at.high + at.highs - t) % at.highs).wait_recv(), 1)
        gain_sum = r.gain_b[0]
        for k in range(1, at.highs):
            gain_sum = gain_sum + r.gain_b[k]
        scatter.drain()
        fore.drain()
        rear.drain()
        each(at.group, lambda t: lead(t).wait_send(), 1)
        each(plane, lambda t: plane_edge(t, place).wait_send(), 1)
        each(at.highs, lambda t: line_edge(t, at.high).wait_send(), 1)
        each(at.n, lambda t: news(t, (at.me + at.n - t) % at.n).wait_recv(), 1)
        each(at.n, lambda t: news(t, at.me).wait_send(), 1)
        sums = jnp.sum(r.inbox[s], axis=0)
        small = jnp.where(lane < 3 * heads, sums, 0.0)
        power = jnp.where(lane == 3 * heads + 1, sums, small * small)
        norm = lane_total(power + total(gain_sum * gain_sum))
        pace = learn_rate * clip_limit / jnp.maximum(jnp.sqrt(norm), clip_limit)
        r.held[...] = r.held[...] - pace * r.acc[...]
        r.params[...] = r.params[...] - pace * small
        r.gain_now[...] = r.gain_now[...] - pace * gain_sum

        @pl.when(s < STEPS - 1)
        def _():
            r.full[at.me] = r.held[...].astype(bf16)
            gather.start()
            own_state()
            open_step()

        r.out_small[pl.ds(s + 1, 1), :] = jnp.broadcast_to(
            lane_total(jnp.where(lane == 3 * heads, sums, 0.0)), (1, LANES)
        )
        return 0

    r.full[at.me] = r.held[...].astype(bf16)
    own_state()
    at.meet()
    gather.start()
    open_step()
    lax.fori_loop(0, STEPS, step, 0)
    r.out_small[0:1, :] = r.params[...]
    r.out_gain[...] = r.gain_now[...]
    r.out_rows[...] = r.held[...]


def finish_kernel(rows, small, gain, losses, new_rows, decay, bias, skip, new_gain):
    heads = decay.shape[1]
    new_rows[...] = rows[...]
    new_gain[...] = gain[...]
    for k, ref in enumerate((decay, bias, skip)):
        ref[...] = small[0:1, k * heads : (k + 1) * heads]
    lane = iota((1, LANES), 1)
    both = jnp.where(lane == 0, small[1:2, :], small[2:3, :])
    losses[...] = both[:, :STEPS]


def call(body, outs, args, scratch=(), far=(), **extra):
    def place(k, a):
        if k in far:
            return pl.BlockSpec(memory_space=pl.ANY)
        return SMEM if a.ndim == 1 else VMEM

    return pl.pallas_call(
        body,
        out_shape=tuple(jax.ShapeDtypeStruct(*o) for o in outs),
        in_specs=[place(k, a) for k, a in enumerate(args)],
        out_specs=tuple([VMEM] * len(outs)),
        scratch_shapes=list(scratch),
        compiler_params=pltpu.CompilerParams(vmem_limit_bytes=LIMIT, **extra),
    )(*args)


def per_device(
    n_dp,
    n_seq,
    head_inputs,
    gate_inputs,
    state_proj,
    time_steps,
    token_ids,
    token_counts,
    teacher_out,
    out_weight,
    decay_log,
    step_bias,
    skip_gain,
    norm_gain,
):
    n = n_dp * n_seq
    x, z, target, raw = head_inputs[0], gate_inputs[0], teacher_out[0], time_steps[0]
    tokens, inner = x.shape
    ns = state_proj.shape[2] // 2
    heads = decay_log.shape[0]
    model = target.shape[1]
    share = out_weight.shape[0]
    group = n_seq // 2
    piece = inner // group
    g = inner // LANES
    cores = 2 if n_dp % 2 == 0 else 1
    ys = n_dp // cores
    highs = 4 if n_seq % 4 == 0 else n_seq
    lows = n_seq // highs
    per_head, tall = ((heads, tokens), f32), (inner, tokens)
    state = ((group, piece, ns), bf16)
    dma = pltpu.SemaphoreType.DMA
    vmem = {
        "x": (x.shape, bf16),
        "z": (z.shape, bf16),
        "target": (target.shape, bf16),
        "proj": (state_proj.shape[1:], bf16),
        "xt": (tall, f32),
        "gate": (tall, f32),
        "mixed": (tall, f32),
        "gated": (tall, f32),
        "ng": (tall, f32),
        "scaled": (tall, bf16),
        "slope": (tall, bf16),
        "normed": (tall, bf16),
        "normed_n": ((tokens, inner), bf16),
        "residual": ((tokens, model), f32),
        "og": ((tokens, model), bf16),
        "upper": ((tokens, tokens), bf16),
        "score": ((tokens, tokens), f32),
        "grid": ((heads, tokens, tokens), bf16),
        "seg": ((16, tokens), f32),
        "sums_c": ((tokens, heads), f32),
        "rate": per_head,
        "bias_w": per_head,
        "skip_w": per_head,
        "width": per_head,
        "sums": per_head,
        "tail": per_head,
        "ending": per_head,
        "entry": per_head,
        "row_dot": per_head,
        "skip_dot": per_head,
        "col_dot": per_head,
        "pulled": per_head,
        "kept": ((heads, ns), f32),
        "root": ((8, tokens), f32),
        "inward": ((8, tokens), f32),
        "gain_w": ((inner, LANES), f32),
        "gain_part": ((inner, LANES), f32),
        "gain_now": ((g, LANES), f32),
        "params": ((1, LANES), f32),
        "held": ((share, model), f32),
        "acc": ((share, model), f32),
        "full": ((n, share, model), bf16),
        "grad": ((n, share, model), bf16),
        "from_core": ((cores * ys, n_seq, share, model), bf16),
        "staged1": ((n // cores, share, model), bf16),
        "from1": ((n // cores, share, model), bf16),
        "staged2": ((n_seq, share, model), bf16),
        "from2": ((n_seq, share, model), bf16),
        "staged3": ((highs, share, model), bf16),
        "from3": ((highs, share, model), bf16),
        "middle": ((2, piece, ns), bf16),
        "b_middle": ((2, piece, ns), bf16),
        "state": state,
        "landed": state,
        "ready": state,
        "entering": state,
        "b_state": state,
        "b_landed": state,
        "b_ready": state,
        "leaving": state,
        "carries": ((group, heads, LANES), f32),
        "gain_a": ((n_dp * lows, g, LANES), f32),
        "gain_b": ((highs, g, LANES), f32),
        "inbox": ((STEPS, n, 1, LANES), f32),
    }
    sems = {
        "l_sem": (4,),
        "w_recv": (n,),
        "wz_send": (highs,),
        "wx_send": (n_seq,),
        "wy_send": (n // cores,),
        "wc_send": (n,),
        "gc_send": (cores * ys,),
        "gc_recv": (cores * ys,),
        "g1_send": (n // cores,),
        "g1_recv": (n // cores,),
        "g2_send": (n_seq,),
        "g2_recv": (n_seq,),
        "g3_send": (highs,),
        "g3_recv": (highs,),
        "m_send": (1,),
        "m_recv": (1,),
        "bm_send": (1,),
        "bm_recv": (1,),
        "pa_send": (n_dp * lows,),
        "pa_recv": (n_dp * lows,),
        "pb_send": (highs,),
        "pb_recv": (highs,),
        "n_send": (n,),
        "n_recv": (n,),
    }
    for name in ("c", "s", "r", "bs", "br"):
        sems[name + "_send"] = (group,)
        sems[name + "_recv"] = (group,)
    given = {
        "counts": token_counts,
        "decay": decay_log.reshape(1, heads),
        "bias": step_bias.reshape(1, heads),
        "skip": skip_gain.reshape(1, heads),
        "gain": norm_gain.reshape(g, LANES),
        "raw_t": raw.T,
        "ids": token_ids,
        "x_in": x,
        "z_in": z,
        "target_in": target,
        "proj_in": state_proj[0],
        "rows": out_weight,
    }
    outs = {
        "out_rows": ((share, model), f32),
        "out_small": ((8, LANES), f32),
        "out_gain": ((g, LANES), f32),
    }
    far = [k for k, name in enumerate(given) if name.endswith("_in")]
    names = [*given, *outs, *vmem, *sems]
    rows, small, gain = call(
        functools.partial(train_kernel, n_dp, n_seq, names),
        outs.values(),
        tuple(given.values()),
        [pltpu.VMEM(*v) for v in vmem.values()] + [dma(v) for v in sems.values()],
        far,
        collective_id=0,
        has_side_effects=True,
    )
    losses, rows, decay, bias, skip, gain = call(
        finish_kernel,
        [
            ((1, STEPS), f32),
            ((share, model), f32),
            ((1, heads), f32),
            ((1, heads), f32),
            ((1, heads), f32),
            ((g, LANES), f32),
        ],
        (rows, small, gain),
    )
    return (
        losses.reshape(STEPS),
        rows,
        decay.reshape(heads),
        bias.reshape(heads),
        skip.reshape(heads),
        gain.reshape(inner),
    )


def solution(mesh):
    in_specs = (
        P("dp", "seq", None),
        P("dp", "seq", None),
        P("dp", "seq", None),
        P("dp", "seq", None),
        P("dp", "seq"),
        P(),
        P("dp", "seq", None),
        P(("dp", "seq"), None),
        P(),
        P(),
        P(),
        P(),
    )
    out_specs = (P(), P(("dp", "seq"), None), P(), P(), P(), P())
    return jax.shard_map(
        functools.partial(per_device, mesh.shape["dp"], mesh.shape["seq"]),
        mesh=mesh,
        in_specs=in_specs,
        out_specs=out_specs,
        check_vma=False,
    )
```

```python
import functools

import jax
import jax.numpy as jnp
from jax import lax
from jax.experimental import pallas as pl
from jax.experimental.pallas import tpu as pltpu
from jax.sharding import PartitionSpec as P

STEPS = 2
norm_floor = 1.0
clip_limit = 1.0
learn_rate = 8.0
log2e = 1.4426950408889634
f32 = jnp.float32
bf16 = jnp.bfloat16
LANES = 128
VMEM = pl.BlockSpec(memory_space=pltpu.VMEM)
SMEM = pl.BlockSpec(memory_space=pltpu.SMEM)
MESH = pl.DeviceIdType.MESH
LIMIT = 60 * 1024 * 1024


def dot(a, b):
    return jnp.dot(a, b, preferred_element_type=f32)


def contract(a, b, da, db):
    return lax.dot_general(a, b, (((da,), (db,)), ((), ())), preferred_element_type=f32)


def iota(shape, axis):
    return lax.broadcasted_iota(jnp.int32, shape, axis)


def fold(a):
    rows, width = a.shape
    return jnp.sum(a.reshape(rows // 8, 8, width), axis=0)


def total(a):
    return jnp.sum(a, axis=0, keepdims=True)


def lane_total(a):
    return jnp.sum(a, axis=1, keepdims=True)


def flat(a):
    k, rows, width = a.shape
    if rows % 16 == 0 or a.dtype == f32:
        return a.reshape(k * rows, width)
    return a.astype(f32).reshape(k * rows, width).astype(a.dtype)


def each(n, body, first=0):
    if n - first <= 3:
        for t in range(first, n):
            body(t)
        return

    def one(t, _):
        body(t)
        return 0

    lax.fori_loop(first, n, one, 0)


def remote(source, target, send, recv, peer):
    return pltpu.make_async_remote_copy(
        src_ref=source,
        dst_ref=target,
        send_sem=send,
        recv_sem=recv,
        device_id=peer,
        device_id_type=MESH,
    )


class Refs:
    def __init__(self, names, refs):
        self.__dict__.update(zip(names, refs))


class Spot:
    def __init__(self, n_dp, n_seq):
        self.n_dp, self.n_seq, self.n = n_dp, n_seq, n_dp * n_seq
        self.cores = 2 if n_dp % 2 == 0 else 1
        self.ys = n_dp // self.cores
        self.highs = 4 if n_seq % 4 == 0 else n_seq
        self.lows = n_seq // self.highs
        self.dp, self.seq = lax.axis_index("dp"), lax.axis_index("seq")
        self.y, self.core = self.dp // self.cores, self.dp % self.cores
        self.high, self.low = self.seq // self.lows, self.seq % self.lows
        self.me = self.dp * n_seq + self.seq
        self.group = n_seq // 2
        self.part, self.spot = self.seq // self.group, self.seq % self.group

    def core_peer(self, t):
        return (self.y * self.cores + (self.core + t) % self.cores, self.seq)

    def y_peer(self, t):
        return (((self.y + t) % self.ys) * self.cores + self.core, self.seq)

    def low_peer(self, t):
        return (self.dp, self.high * self.lows + (self.low + t) % self.lows)

    def high_peer(self, t):
        return (self.dp, ((self.high + t) % self.highs) * self.lows + self.low)

    def group_peer(self, t):
        return (self.dp, self.part * self.group + (self.spot + t) % self.group)

    def other_half(self):
        return (self.dp, (self.seq + self.group) % self.n_seq)

    def any_peer(self, t):
        to = (self.me + t) % self.n
        return (to // self.n_seq, to % self.n_seq)

    def plane_peer(self, t):
        to = (self.dp * self.lows + self.low + t) % (self.n_dp * self.lows)
        return (to // self.lows, self.high * self.lows + to % self.lows)

    def chunk(self, y, high, low):
        return (y * self.cores + self.core) * self.n_seq + high * self.lows + low

    def near(self):
        return [
            (self.highs, self.high_peer),
            (self.group, self.group_peer),
            (2, lambda t: self.other_half()),
            (self.n_dp * self.lows, self.plane_peer),
        ]

    def greet(self):
        barrier = pltpu.get_barrier_semaphore()
        for count, peer in self.near():
            each(
                count,
                lambda t, peer=peer: pl.semaphore_signal(
                    barrier, inc=1, device_id=peer(t), device_id_type=MESH
                ),
                1,
            )

    def meet(self):
        count = sum(count - 1 for count, _ in self.near())
        pl.semaphore_wait(pltpu.get_barrier_semaphore(), count)


def to_column(row, k, heads):
    sub, lane = iota((heads, LANES), 0), iota((heads, LANES), 1)
    return lane_total(jnp.where(lane == k * heads + sub, row, 0.0))


def to_row(column, k):
    heads = column.shape[0]
    sub, lane = iota((heads, LANES), 0), iota((heads, LANES), 1)
    return total(jnp.where(lane == k * heads + sub, column, 0.0))


def accumulate(a, upper, axis):
    rows = a.shape[0]
    high = a.astype(bf16)
    rest = a - high.astype(f32)
    mid = rest.astype(bf16)
    low = (rest - mid.astype(f32)).astype(bf16)
    out = contract(jnp.concatenate([high, mid, low], axis=0), upper, 1, axis)
    return out[:rows] + out[rows : 2 * rows] + out[2 * rows :]


class Gather:
    def __init__(self, at, r):
        self.at, self.r = at, r

    def push(self, chunk, send, peer):
        r = self.r
        return remote(r.full.at[chunk], r.full.at[chunk], send, r.w_recv.at[chunk], peer)

    def arrived(self, chunk):
        self.push(chunk, self.r.wz_send.at[0], self.at.core_peer(1)).wait_recv()

    def high_edge(self, t):
        return self.push(self.at.me, self.r.wz_send.at[t], self.at.high_peer(t))

    def low_edge(self, t, high):
        at = self.at
        chunk = at.chunk(at.y, high, at.low)
        return self.push(chunk, self.r.wx_send.at[t * at.highs + high], at.low_peer(t))

    def y_edge(self, t, high, low):
        at = self.at
        send = self.r.wy_send.at[(t * at.highs + high) * at.lows + low]
        return self.push(at.chunk(at.y, high, low), send, at.y_peer(t))

    def core_edge(self, t, y, seq):
        at = self.at
        send = self.r.wc_send.at[(t * at.ys + y) * at.n_seq + seq]
        return self.push((y * at.cores + at.core) * at.n_seq + seq, send, at.core_peer(t))

    def onward(self, y, high, low, to_low, to_y):
        at = self.at
        if to_low:
            each(at.lows, lambda t: self.low_edge(t, high).start(), 1)
        if to_y:
            each(at.ys, lambda t: self.y_edge(t, high, low).start(), 1)
        each(at.cores, lambda t: self.core_edge(t, y, high * at.lows + low).start(), 1)

    def start(self):
        at = self.at
        each(at.highs, lambda t: self.high_edge(t).start(), 1)
        self.onward(at.y, at.high, at.low, True, True)

    def from_high(self):
        at = self.at

        def one(t):
            high = (at.high + at.highs - t) % at.highs
            self.arrived(at.chunk(at.y, high, at.low))
            self.onward(at.y, high, at.low, True, True)

        each(at.highs, one, 1)

    def from_low(self, u):
        at = self.at
        high = (at.high + at.highs - u) % at.highs

        def pick(t):
            low = (at.low + at.lows - t) % at.lows
            self.arrived(at.chunk(at.y, high, low))
            self.onward(at.y, high, low, False, True)

        each(at.lows, pick, 1)

    def from_y(self):
        at = self.at

        def one(t, v):
            y = (at.y + at.ys - t) % at.ys
            high = (at.high + at.highs - v % at.highs) % at.highs
            low = (at.low + v // at.highs) % at.lows
            self.arrived(at.chunk(y, high, low))
            self.onward(y, high, low, False, False)

        each(at.ys, lambda t: each(at.n_seq, lambda v: one(t, v)), 1)

    def from_core(self):
        at = self.at

        def one(t, v):
            core = (at.core + t) % at.cores
            self.arrived(((v // at.n_seq) * at.cores + core) * at.n_seq + v % at.n_seq)

        each(at.cores, lambda t: each(at.ys * at.n_seq, lambda v: one(t, v)), 1)

    def drain(self):
        at = self.at
        each(at.highs, lambda t: self.high_edge(t).wait_send(), 1)
        each(at.lows, lambda t: each(at.highs, lambda u: self.low_edge(t, u).wait_send()), 1)
        each(
            at.ys,
            lambda t: each(
                at.n_seq, lambda v: self.y_edge(t, v // at.lows, v % at.lows).wait_send()
            ),
            1,
        )
        each(
            at.cores,
            lambda t: each(
                at.ys * at.n_seq,
                lambda v: self.core_edge(t, v // at.n_seq, v % at.n_seq).wait_send(),
            ),
            1,
        )


class Scatter:
    def __init__(self, at, r):
        self.at, self.r = at, r

    def core_edge(self, t, y):
        at, r = self.at, self.r
        dp = y * at.cores + (at.core + t) % at.cores
        slot = t * at.ys + y
        return remote(
            r.grad.at[pl.ds(dp * at.n_seq, at.n_seq)], r.from_core.at[slot],
            r.gc_send.at[slot], r.gc_recv.at[slot], at.core_peer(t),
        )

    def y_edge(self, t, high, low):
        at, r = self.at, self.r
        slot = (t * at.highs + high) * at.lows + low
        return remote(
            r.staged1.at[slot], r.from1.at[slot],
            r.g1_send.at[slot], r.g1_recv.at[slot], at.y_peer(t),
        )

    def low_edge(self, t, high):
        at, r = self.at, self.r
        slot = t * at.highs + high
        return remote(
            r.staged2.at[slot], r.from2.at[slot],
            r.g2_send.at[slot], r.g2_recv.at[slot], at.low_peer(t),
        )

    def high_edge(self, t):
        at, r = self.at, self.r
        return remote(
            r.staged3.at[t], r.from3.at[t], r.g3_send.at[t], r.g3_recv.at[t], at.high_peer(t)
        )

    def chip_sum(self, y, high, low):
        at, r = self.at, self.r
        acc = r.grad[at.chunk(y, high, low)].astype(f32)
        for t in range(1, at.cores):
            acc = acc + r.from_core[t * at.ys + y, high * at.lows + low].astype(f32)
        return acc

    def y_sum(self, high, low):
        at, r = self.at, self.r
        acc = self.chip_sum(at.y, high, low)
        for t in range(1, at.ys):
            self.y_edge(t, high, low).wait_recv()
            acc = acc + r.from1[(t * at.highs + high) * at.lows + low].astype(f32)
        return acc

    def low_sum(self, high):
        at, r = self.at, self.r
        acc = self.y_sum(high, at.low)
        for t in range(1, at.lows):
            self.low_edge(t, high).wait_recv()
            acc = acc + r.from2[t * at.highs + high].astype(f32)
        return acc

    def from_core(self, u):
        at = self.at
        each(at.cores, lambda t: self.core_edge(t, (at.y + u) % at.ys).wait_recv(), 1)

    def to_y(self):
        at, r = self.at, self.r
        each(at.ys, self.from_core, 1)

        def one(t, v):
            low = (at.low + 1 + v // at.highs) % at.lows
            high = (at.high + 1 + v) % at.highs
            acc = self.chip_sum((at.y + t) % at.ys, high, low)
            r.staged1[(t * at.highs + high) * at.lows + low] = acc.astype(bf16)
            self.y_edge(t, high, low).start()

        each(at.ys, lambda t: each(at.n_seq, lambda v: one(t, v)), 1)

    def to_low(self, u):
        at, r = self.at, self.r
        high = (at.high + 1 + u) % at.highs

        def one(t):
            low = (at.low + t) % at.lows
            r.staged2[t * at.highs + high] = self.y_sum(high, low).astype(bf16)
            self.low_edge(t, high).start()

        each(at.lows, one, 1)

    def to_high(self, t):
        at, r = self.at, self.r
        r.staged3[t] = self.low_sum((at.high + t) % at.highs).astype(bf16)
        self.high_edge(t).start()

    def finish(self):
        at, r = self.at, self.r
        acc = self.low_sum(at.high)
        each(at.highs, lambda t: self.high_edge(t).wait_recv(), 1)
        for t in range(1, at.highs):
            acc = acc + r.from3[t].astype(f32)
        r.acc[...] = acc
        return lane_total(total(fold(acc * acc)))

    def drain(self):
        at = self.at
        for t in range(1, at.cores):
            each(at.ys, lambda y: self.core_edge(t, y).wait_send())
        each(
            at.ys,
            lambda t: each(
                at.n_seq, lambda v: self.y_edge(t, v // at.lows, v % at.lows).wait_send()
            ),
            1,
        )
        each(at.lows, lambda t: each(at.highs, lambda u: self.low_edge(t, u).wait_send()), 1)
        each(at.highs, lambda t: self.high_edge(t).wait_send(), 1)


class Exchange:
    def __init__(self, at, reverse, state, landed, ready, entering, middle, sems):
        self.at, self.reverse = at, reverse
        self.state, self.landed, self.ready, self.entering = state, landed, ready, entering
        self.middle = middle
        self.s_send, self.s_recv, self.r_send, self.r_recv, self.m_send, self.m_recv = sems
        self.leader = 1 if reverse else 0

    def back(self, t):
        return (self.at.spot + self.at.group - t) % self.at.group

    def first(self, t):
        p = (self.at.spot + t) % self.at.group
        return remote(
            self.state.at[p], self.landed.at[self.at.spot],
            self.s_send.at[t], self.s_recv.at[t], self.at.group_peer(t),
        )

    def first_in(self, t):
        p = self.back(t)
        return remote(
            self.state.at[p], self.landed.at[p],
            self.s_send.at[t], self.s_recv.at[t], self.at.group_peer(t),
        )

    def second(self, t):
        p = (self.at.spot + t) % self.at.group
        return remote(
            self.ready.at[p], self.entering.at[self.at.spot],
            self.r_send.at[t], self.r_recv.at[t], self.at.group_peer(t),
        )

    def second_in(self, t):
        p = self.back(t)
        return remote(
            self.ready.at[p], self.entering.at[p],
            self.r_send.at[t], self.r_recv.at[t], self.at.group_peer(t),
        )

    def across(self):
        return remote(
            self.middle.at[0], self.middle.at[1],
            self.m_send.at[0], self.m_recv.at[0], self.at.other_half(),
        )

    def start(self):
        at = self.at
        each(at.group, lambda t: self.first(t).start(), 1)
        self.landed[at.spot] = self.state[at.spot]

    def lead(self, carries, size):
        @pl.when(self.at.part == self.leader)
        def _():
            self.turn(carries, size, True)

    def follow(self, carries, size):
        @pl.when(self.at.part != self.leader)
        def _():
            self.turn(carries, size, False)

    def turn(self, carries, size, leads):
        at = self.at
        mine, group = at.spot, at.group
        each(group, lambda t: self.first_in(t).wait_recv(), 1)
        if not leads:
            self.across().wait_recv()
        piece = self.state.shape[1]
        per = piece // size
        order = list(range(group))
        if self.reverse:
            order.reverse()
        for q in range(per):
            rows = slice(q * size, (q + 1) * size)
            if leads:
                running = jnp.zeros((size, self.state.shape[2]), f32)
            else:
                running = self.middle[1, rows, :].astype(f32)
            for n, d in enumerate(order):
                self.ready[d, rows, :] = running.astype(bf16)
                if leads or n < group - 1:
                    kept = carries[d, pl.ds(mine * per + q, 1), :]
                    running = kept * running + self.landed[d, rows, :].astype(f32)
            if leads:
                self.middle[0, rows, :] = running.astype(bf16)
        if leads:
            self.across().start()
        each(group, lambda t: self.second(t).start(), 1)
        self.entering[mine] = self.ready[mine]

    def finish(self):
        each(self.at.group, lambda t: self.second_in(t).wait_recv(), 1)

    def drain(self):
        each(self.at.group, lambda t: self.first(t).wait_send(), 1)
        each(self.at.group, lambda t: self.second(t).wait_send(), 1)

        @pl.when(self.at.part == self.leader)
        def _():
            self.across().wait_send()


def train_kernel(n_dp, n_seq, names, *refs):
    r = Refs(names, refs)
    at = Spot(n_dp, n_seq)
    inner, tokens = r.xt.shape
    heads = r.decay.shape[1]
    size = inner // heads
    ns = r.proj.shape[1] // 2
    share, model = r.rows.shape
    g = inner // LANES
    blocks = tokens // LANES
    head_rows = [slice(h * size, (h + 1) * size) for h in range(heads)]
    gather, scatter = Gather(at, r), Scatter(at, r)
    fore = Exchange(
        at, False, r.state, r.landed, r.ready, r.entering, r.middle,
        (r.s_send, r.s_recv, r.r_send, r.r_recv, r.m_send, r.m_recv),
    )
    rear = Exchange(
        at, True, r.b_state, r.b_landed, r.b_ready, r.leaving, r.b_middle,
        (r.bs_send, r.bs_recv, r.br_send, r.br_recv, r.bm_send, r.bm_recv),
    )
    b, c = slice(0, ns), slice(ns, 2 * ns)

    def wide(column):
        return jnp.concatenate([column] * blocks, axis=1)

    def lead(t):
        return remote(
            r.carries.at[at.spot], r.carries.at[at.spot],
            r.c_send.at[t], r.c_recv.at[t], at.group_peer(t),
        )

    def lead_in(t):
        p = (at.spot + at.group - t) % at.group
        return remote(
            r.carries.at[p], r.carries.at[p], r.c_send.at[t], r.c_recv.at[t], at.group_peer(t)
        )

    plane = n_dp * at.lows
    place = at.dp * at.lows + at.low

    def plane_edge(t, slot):
        return remote(
            r.gain_a.at[place], r.gain_a.at[slot],
            r.pa_send.at[t], r.pa_recv.at[t], at.plane_peer(t),
        )

    def line_edge(t, slot):
        return remote(
            r.gain_b.at[at.high], r.gain_b.at[slot],
            r.pb_send.at[t], r.pb_recv.at[t], at.high_peer(t),
        )

    def load(k, ref, to):
        return pltpu.make_async_copy(ref, to, r.l_sem.at[k])

    loads = [
        load(0, r.x_in, r.x), load(1, r.proj_in, r.proj),
        load(2, r.z_in, r.z), load(3, r.target_in, r.target),
    ]
    at.greet()
    for one in loads:
        one.start()
    r.held[...] = r.rows[...]
    for k, ref in enumerate((r.decay, r.bias, r.skip)):
        sub, lane = iota((heads, heads), 0), iota((heads, heads), 1)
        own = lane_total(jnp.where(sub == lane, ref[...], 0.0))
        row = to_row(own, k)
        packed = row if k == 0 else packed + row
    r.params[...] = packed
    r.gain_now[...] = r.gain[...]
    r.upper[...] = (iota((tokens, tokens), 0) <= iota((tokens, tokens), 1)).astype(bf16)
    loads[0].wait()
    for k in range(g):
        cols = slice(k * LANES, (k + 1) * LANES)
        r.xt[cols, :] = r.x[:, cols].astype(f32).T
    loads[1].wait()
    stop = jnp.where(r.ids[...] == 0, 1.0, 0.0)
    r.seg[...] = dot(jnp.broadcast_to(stop, (16, tokens)).astype(bf16), r.upper[...])

    def prepare():
        loads[2].wait()
        loads[3].wait()
        seg_c = r.seg[...].T[:, 0:1]
        raw = contract(r.proj[:, b], r.proj[:, c], 1, 1)
        open_to = (seg_c == r.seg[0:1, :]) & (
            iota((tokens, tokens), 0) <= iota((tokens, tokens), 1)
        )
        r.score[...] = jnp.where(open_to, raw, 0.0)
        for k in range(g):
            cols = slice(k * LANES, (k + 1) * LANES)
            zt = r.z[:, cols].astype(f32).T
            r.gate[cols, :] = zt * jax.nn.sigmoid(zt)

    def forward_head(h):
        rows = head_rows[h]
        for jb in range(blocks):
            js = slice(jb * LANES, (jb + 1) * LANES)
            left = r.sums_c[js, h : h + 1]
            for ib in range(jb, blocks):
                cs = slice(ib * LANES, (ib + 1) * LANES)
                gap = r.sums[h : h + 1, cs] - left
                if ib == jb:
                    gap = jnp.minimum(gap, 0.0)
                r.grid[h, js, cs] = (jnp.exp2(gap) * r.score[js, cs]).astype(bf16)
        for ib in range(blocks):
            end = (ib + 1) * LANES
            cs = slice(ib * LANES, end)
            r.mixed[rows, cs] = dot(r.scaled[rows, :end], r.grid[h, :end, cs])

    def backward_head(h):
        rows = head_rows[h]
        for jb in range(blocks):
            at_j = jb * LANES
            js = slice(at_j, at_j + LANES)
            part = contract(r.slope[rows, at_j:], r.grid[h, js, at_j:], 1, 1)
            r.col_dot[h : h + 1, js] = total(part * r.xt[rows, js])

    def own_state():
        packed = r.params[...]
        rate = -jnp.exp(jnp.broadcast_to(to_column(packed, 0, heads), (heads, tokens)))
        bias = jnp.broadcast_to(to_column(packed, 1, heads), (heads, tokens))
        w = jax.nn.softplus(r.raw_t[...] + bias)
        sums = accumulate(w * (rate * log2e), r.upper[...], 0)
        seg = r.seg[...][:heads]
        final = sums[:, tokens - 1 : tokens]
        last = seg[:, tokens - 1 : tokens]
        tail = jnp.where(seg == last, jnp.exp2(final - sums), 0.0)
        r.rate[...] = rate
        r.bias_w[...] = bias
        r.width[...] = w
        r.sums[...] = sums
        r.tail[...] = tail
        r.ending[...] = w * tail
        r.entry[...] = jnp.where(seg == 0.0, jnp.exp2(sums), 0.0)
        r.carries[at.spot] = jnp.broadcast_to(
            jnp.where(last == 0.0, jnp.exp2(final), 0.0), (heads, LANES)
        )
        for h in range(heads):
            rows = head_rows[h]
            r.slope[rows, :] = (r.xt[rows, :] * r.ending[h : h + 1, :]).astype(bf16)
        ended = dot(r.slope[...], r.proj[:, b])
        r.state[...] = ended.reshape(r.state.shape).astype(bf16)

    def open_step():
        each(at.group, lambda t: lead(t).start(), 1)
        fore.start()

    def step(s, _):
        r.sums_c[...] = r.sums[...].T
        for h in range(heads):
            rows = head_rows[h]
            r.scaled[rows, :] = (r.xt[rows, :] * r.width[h : h + 1, :]).astype(bf16)

        @pl.when(s == 0)
        def _():
            prepare()

        for k in range(g):
            row = jnp.broadcast_to(r.gain_now[k : k + 1, :], (LANES, LANES))
            r.gain_w[k * LANES : (k + 1) * LANES, :] = row.T
        cut = heads // 8
        marks = [slice(k * cut, (k + 1) * cut) for k in range(8)]

        def forward(k):
            for h in range(heads)[marks[k]]:
                forward_head(h)

        def backward(k):
            for h in range(heads)[marks[k]]:
                backward_head(h)

        forward(0)
        gather.from_low(0)
        forward(1)
        gather.from_high()
        each(at.group, lambda t: lead_in(t).wait_recv(), 1)
        fore.lead(r.carries, size)
        for u in range(1, at.highs):
            gather.from_low(u)
        for k in range(2, 5):
            forward(k)
        fore.follow(r.carries, size)
        for k in range(5, 8):
            forward(k)
        gather.from_y()
        fore.finish()

        passed = contract(flat(r.entering[...]), r.proj[:, c], 1, 1)
        skip = jnp.broadcast_to(to_column(r.params[...], 2, heads), (heads, tokens))
        r.skip_w[...] = skip
        power = jnp.zeros((8, tokens), f32)
        for h in range(heads):
            rows = head_rows[h]
            y = r.mixed[rows, :] + passed[rows, :] * r.entry[h : h + 1, :]
            r.mixed[rows, :] = y
            gated = (y + r.skip_w[h : h + 1, :] * r.xt[rows, :]) * r.gate[rows, :]
            r.gated[rows, :] = gated
            power = power + fold(gated * gated)
        root = lax.rsqrt(total(power) * (1.0 / inner) + norm_floor)
        r.root[...] = jnp.broadcast_to(root, r.root.shape)
        for k in range(g):
            rows = slice(k * LANES, (k + 1) * LANES)
            normed = r.gated[rows, :] * wide(r.gain_w[rows, :]) * r.root[0:1, :]
            r.normed[rows, :] = normed.astype(bf16)
            r.normed_n[:, rows] = normed.T.astype(bf16)

        gather.from_core()
        r.residual[...] = dot(r.normed_n[...], flat(r.full[...]))
        count = r.counts[0]
        for k in range(1, n_dp):
            count = count + r.counts[k]
        share_of = 1.0 / (model * count.astype(f32))
        limit = r.counts[at.dp] - at.seq * tokens
        lost = jnp.zeros((8, model), f32)
        step_rows = 32
        for q in range(tokens // step_rows):
            rows = slice(q * step_rows, (q + 1) * step_rows)
            scored = iota((step_rows, model), 0) + q * step_rows < limit
            gap = jnp.where(scored, r.residual[rows, :] - r.target[rows, :].astype(f32), 0.0)
            lost = lost + fold(gap * gap)
            r.og[rows, :] = (gap * (2.0 * share_of)).astype(bf16)
        loss = lane_total(total(lost)) * share_of

        def weight_part(t, y):
            dp = y * at.cores + (at.core + t) % at.cores
            width = n_seq * share
            left = r.normed[pl.ds(pl.multiple_of(dp * width, width), width), :]
            out = dot(left, r.og[...])
            r.grad[pl.ds(dp * n_seq, n_seq)] = out.reshape(n_seq, share, model).astype(bf16)
            if t > 0:
                scatter.core_edge(t, y).start()

        for t in range(1, at.cores):
            for u in range(at.ys):
                weight_part(t, (at.y + 1 + u) % at.ys)
        for u in range(at.ys):
            weight_part(0, (at.y + 1 + u) % at.ys)
        r.ng[...] = contract(flat(r.full[...]), r.og[...], 1, 1)
        scatter.to_y()
        inward = jnp.zeros((8, tokens), f32)
        for h in range(heads):
            rows = head_rows[h]
            lifted = r.ng[rows, :] * r.gated[rows, :]
            inward = inward + fold(lifted * wide(r.gain_w[rows, :]))
            lifted = lifted * r.root[0:1, :]
            part = lifted[:, :LANES]
            for k in range(1, blocks):
                part = part + lifted[:, k * LANES : (k + 1) * LANES]
            r.gain_part[rows, :] = part
        root = r.root[0:1, :]
        inward = total(inward) * (root * root * root * (1.0 / inner))
        r.inward[...] = jnp.broadcast_to(inward, r.inward.shape)
        for h in range(heads):
            rows = head_rows[h]
            dy = r.ng[rows, :] * wide(r.gain_w[rows, :]) * r.root[0:1, :]
            dy = (dy - r.gated[rows, :] * r.inward[0:1, :]) * r.gate[rows, :]
            r.row_dot[h : h + 1, :] = total(dy * r.mixed[rows, :])
            r.skip_dot[h : h + 1, :] = total(dy * r.xt[rows, :])
            r.slope[rows, :] = dy.astype(bf16)
            r.scaled[rows, :] = (dy * r.entry[h : h + 1, :]).astype(bf16)
        pulled = dot(r.scaled[...], r.proj[:, c])
        r.b_state[...] = pulled.reshape(r.b_state.shape).astype(bf16)
        rear.start()
        backward(0)
        scatter.from_core(0)
        for u in range(at.highs):
            scatter.to_low(u)
            if u < 3:
                backward(u + 1)
            if u == 2:
                rear.lead(r.carries, size)
        backward(4)
        for k in range(g):
            rows = slice(k * LANES, (k + 1) * LANES)
            r.gain_a[place, k : k + 1, :] = total(r.gain_part[rows, :].T)
        each(plane, lambda t: plane_edge(t, place).start(), 1)
        for t in range(1, at.highs):
            scatter.to_high(t)
        rear.follow(r.carries, size)
        for k in range(5, 8):
            backward(k)
        each(plane, lambda t: plane_edge(t, (place + plane - t) % plane).wait_recv(), 1)
        gain_sum = r.gain_a[0]
        for k in range(1, plane):
            gain_sum = gain_sum + r.gain_a[k]
        r.gain_b[at.high] = gain_sum
        each(at.highs, lambda t: line_edge(t, at.high).start(), 1)
        gather.drain()
        square = scatter.finish()
        rear.finish()

        after = flat(r.leaving[...])
        moved = contract(after, r.proj[:, b], 1, 1)
        for h in range(heads):
            rows = head_rows[h]
            r.pulled[h : h + 1, :] = total(moved[rows, :] * r.xt[rows, :])
        piece = r.leaving.shape[1]
        for h in range(heads):
            p, q = (h * size) // piece, (h * size) % piece
            own = r.leaving[p, q : q + size, :].astype(f32)
            own = own * r.entering[p, q : q + size, :].astype(f32)
            r.kept[h : h + 1, :] = total(own)
        drawn = r.pulled[...] * r.tail[...]
        w, rate = r.width[...], r.rate[...]
        col = r.col_dot[...] + drawn
        d_final = lane_total(w * drawn) + lane_total(r.kept[...] * r.carries[at.spot])
        d_rate = accumulate(r.row_dot[...] - w * col, r.upper[...], 1) + d_final
        d_width = (col + rate * d_rate) * jax.nn.sigmoid(r.raw_t[...] + r.bias_w[...])
        message = (
            to_row(lane_total(rate * d_rate * w), 0)
            + to_row(lane_total(d_width), 1)
            + to_row(lane_total(r.skip_dot[...]), 2)
        )
        lane = iota((1, LANES), 1)
        message = message + jnp.where(lane == 3 * heads, loss, 0.0)
        message = message + jnp.where(lane == 3 * heads + 1, square, 0.0)
        r.inbox[s, at.me] = message

        def news(t, slot):
            return remote(
                r.inbox.at[s, at.me], r.inbox.at[s, slot],
                r.n_send.at[t], r.n_recv.at[t], at.any_peer(t),
            )

        each(at.n, lambda t: news(t, at.me).start(), 1)
        each(at.highs, lambda t: line_edge(t, (at.high + at.highs - t) % at.highs).wait_recv(), 1)
        gain_sum = r.gain_b[0]
        for k in range(1, at.highs):
            gain_sum = gain_sum + r.gain_b[k]
        scatter.drain()
        fore.drain()
        rear.drain()
        each(at.group, lambda t: lead(t).wait_send(), 1)
        each(plane, lambda t: plane_edge(t, place).wait_send(), 1)
        each(at.highs, lambda t: line_edge(t, at.high).wait_send(), 1)
        each(at.n, lambda t: news(t, (at.me + at.n - t) % at.n).wait_recv(), 1)
        each(at.n, lambda t: news(t, at.me).wait_send(), 1)
        sums = jnp.sum(r.inbox[s], axis=0)
        small = jnp.where(lane < 3 * heads, sums, 0.0)
        power = jnp.where(lane == 3 * heads + 1, sums, small * small)
        norm = lane_total(power + total(gain_sum * gain_sum))
        pace = learn_rate * clip_limit / jnp.maximum(jnp.sqrt(norm), clip_limit)
        r.held[...] = r.held[...] - pace * r.acc[...]
        r.params[...] = r.params[...] - pace * small
        r.gain_now[...] = r.gain_now[...] - pace * gain_sum

        @pl.when(s < STEPS - 1)
        def _():
            r.full[at.me] = r.held[...].astype(bf16)
            gather.start()
            own_state()
            open_step()

        r.out_small[pl.ds(s + 1, 1), :] = jnp.broadcast_to(
            lane_total(jnp.where(lane == 3 * heads, sums, 0.0)), (1, LANES)
        )
        return 0

    r.full[at.me] = r.held[...].astype(bf16)
    own_state()
    at.meet()
    gather.start()
    open_step()
    lax.fori_loop(0, STEPS, step, 0)
    r.out_small[0:1, :] = r.params[...]
    r.out_gain[...] = r.gain_now[...]
    r.out_rows[...] = r.held[...]


def finish_kernel(rows, small, gain, losses, new_rows, decay, bias, skip, new_gain):
    heads = decay.shape[1]
    new_rows[...] = rows[...]
    new_gain[...] = gain[...]
    for k, ref in enumerate((decay, bias, skip)):
        ref[...] = small[0:1, k * heads : (k + 1) * heads]
    lane = iota((1, LANES), 1)
    both = jnp.where(lane == 0, small[1:2, :], small[2:3, :])
    losses[...] = both[:, :STEPS]


def call(body, outs, args, scratch=(), far=(), **extra):
    def place(k, a):
        if k in far:
            return pl.BlockSpec(memory_space=pl.ANY)
        return SMEM if a.ndim == 1 else VMEM

    return pl.pallas_call(
        body,
        out_shape=tuple(jax.ShapeDtypeStruct(*o) for o in outs),
        in_specs=[place(k, a) for k, a in enumerate(args)],
        out_specs=tuple([VMEM] * len(outs)),
        scratch_shapes=list(scratch),
        compiler_params=pltpu.CompilerParams(vmem_limit_bytes=LIMIT, **extra),
    )(*args)


def per_device(
    n_dp,
    n_seq,
    head_inputs,
    gate_inputs,
    state_proj,
    time_steps,
    token_ids,
    token_counts,
    teacher_out,
    out_weight,
    decay_log,
    step_bias,
    skip_gain,
    norm_gain,
):
    n = n_dp * n_seq
    x, z, target, raw = head_inputs[0], gate_inputs[0], teacher_out[0], time_steps[0]
    tokens, inner = x.shape
    ns = state_proj.shape[2] // 2
    heads = decay_log.shape[0]
    model = target.shape[1]
    share = out_weight.shape[0]
    group = n_seq // 2
    piece = inner // group
    g = inner // LANES
    cores = 2 if n_dp % 2 == 0 else 1
    ys = n_dp // cores
    highs = 4 if n_seq % 4 == 0 else n_seq
    lows = n_seq // highs
    per_head, tall = ((heads, tokens), f32), (inner, tokens)
    state = ((group, piece, ns), bf16)
    dma = pltpu.SemaphoreType.DMA
    vmem = {
        "x": (x.shape, bf16),
        "z": (z.shape, bf16),
        "target": (target.shape, bf16),
        "proj": (state_proj.shape[1:], bf16),
        "xt": (tall, f32),
        "gate": (tall, f32),
        "mixed": (tall, f32),
        "gated": (tall, f32),
        "ng": (tall, f32),
        "scaled": (tall, bf16),
        "slope": (tall, bf16),
        "normed": (tall, bf16),
        "normed_n": ((tokens, inner), bf16),
        "residual": ((tokens, model), f32),
        "og": ((tokens, model), bf16),
        "upper": ((tokens, tokens), bf16),
        "score": ((tokens, tokens), f32),
        "grid": ((heads, tokens, tokens), bf16),
        "seg": ((16, tokens), f32),
        "sums_c": ((tokens, heads), f32),
        "rate": per_head,
        "bias_w": per_head,
        "skip_w": per_head,
        "width": per_head,
        "sums": per_head,
        "tail": per_head,
        "ending": per_head,
        "entry": per_head,
        "row_dot": per_head,
        "skip_dot": per_head,
        "col_dot": per_head,
        "pulled": per_head,
        "kept": ((heads, ns), f32),
        "root": ((8, tokens), f32),
        "inward": ((8, tokens), f32),
        "gain_w": ((inner, LANES), f32),
        "gain_part": ((inner, LANES), f32),
        "gain_now": ((g, LANES), f32),
        "params": ((1, LANES), f32),
        "held": ((share, model), f32),
        "acc": ((share, model), f32),
        "full": ((n, share, model), bf16),
        "grad": ((n, share, model), bf16),
        "from_core": ((cores * ys, n_seq, share, model), bf16),
        "staged1": ((n // cores, share, model), bf16),
        "from1": ((n // cores, share, model), bf16),
        "staged2": ((n_seq, share, model), bf16),
        "from2": ((n_seq, share, model), bf16),
        "staged3": ((highs, share, model), bf16),
        "from3": ((highs, share, model), bf16),
        "middle": ((2, piece, ns), bf16),
        "b_middle": ((2, piece, ns), bf16),
        "state": state,
        "landed": state,
        "ready": state,
        "entering": state,
        "b_state": state,
        "b_landed": state,
        "b_ready": state,
        "leaving": state,
        "carries": ((group, heads, LANES), f32),
        "gain_a": ((n_dp * lows, g, LANES), f32),
        "gain_b": ((highs, g, LANES), f32),
        "inbox": ((STEPS, n, 1, LANES), f32),
    }
    sems = {
        "l_sem": (4,),
        "w_recv": (n,),
        "wz_send": (highs,),
        "wx_send": (n_seq,),
        "wy_send": (n // cores,),
        "wc_send": (n,),
        "gc_send": (cores * ys,),
        "gc_recv": (cores * ys,),
        "g1_send": (n // cores,),
        "g1_recv": (n // cores,),
        "g2_send": (n_seq,),
        "g2_recv": (n_seq,),
        "g3_send": (highs,),
        "g3_recv": (highs,),
        "m_send": (1,),
        "m_recv": (1,),
        "bm_send": (1,),
        "bm_recv": (1,),
        "pa_send": (n_dp * lows,),
        "pa_recv": (n_dp * lows,),
        "pb_send": (highs,),
        "pb_recv": (highs,),
        "n_send": (n,),
        "n_recv": (n,),
    }
    for name in ("c", "s", "r", "bs", "br"):
        sems[name + "_send"] = (group,)
        sems[name + "_recv"] = (group,)
    given = {
        "counts": token_counts,
        "decay": decay_log.reshape(1, heads),
        "bias": step_bias.reshape(1, heads),
        "skip": skip_gain.reshape(1, heads),
        "gain": norm_gain.reshape(g, LANES),
        "raw_t": raw.T,
        "ids": token_ids,
        "x_in": x,
        "z_in": z,
        "target_in": target,
        "proj_in": state_proj[0],
        "rows": out_weight,
    }
    outs = {
        "out_rows": ((share, model), f32),
        "out_small": ((8, LANES), f32),
        "out_gain": ((g, LANES), f32),
    }
    far = [k for k, name in enumerate(given) if name.endswith("_in")]
    names = [*given, *outs, *vmem, *sems]
    rows, small, gain = call(
        functools.partial(train_kernel, n_dp, n_seq, names),
        outs.values(),
        tuple(given.values()),
        [pltpu.VMEM(*v) for v in vmem.values()] + [dma(v) for v in sems.values()],
        far,
        collective_id=0,
        has_side_effects=True,
    )
    losses, rows, decay, bias, skip, gain = call(
        finish_kernel,
        [
            ((1, STEPS), f32),
            ((share, model), f32),
            ((1, heads), f32),
            ((1, heads), f32),
            ((1, heads), f32),
            ((g, LANES), f32),
        ],
        (rows, small, gain),
    )
    return (
        losses.reshape(STEPS),
        rows,
        decay.reshape(heads),
        bias.reshape(heads),
        skip.reshape(heads),
        gain.reshape(inner),
    )


def solution(mesh):
    in_specs = (
        P("dp", "seq", None),
        P("dp", "seq", None),
        P("dp", "seq", None),
        P("dp", "seq", None),
        P("dp", "seq"),
        P(),
        P("dp", "seq", None),
        P(("dp", "seq"), None),
        P(),
        P(),
        P(),
        P(),
    )
    out_specs = (P(), P(("dp", "seq"), None), P(), P(), P(), P())
    return jax.shard_map(
        functools.partial(per_device, mesh.shape["dp"], mesh.shape["seq"]),
        mesh=mesh,
        in_specs=in_specs,
        out_specs=out_specs,
        check_vma=False,
    )
```
